256 devices in a mesh: gx: 8 (over z), gy: 8 (over x, core), gz: 4 (over y).
Axes of the slice: x: 4, y: 4, z: 8, core: 2. Of those that a mesh axis runs over, the one named last changes fastest.
Arguments:
- displacement: float32 [3, 64, 128, 512], P(None, 'gx', 'gy', 'gz'), may hold values from -100 to 100
- density: float32 [64, 128, 512], P('gx', 'gy', 'gz'), may hold values from 0.1 to 1
Outputs:
- aggregate: float32 [], replicated
- adjoint: float32 [3, 64, 128, 512], P(None, 'gx', 'gy', 'gz')
- sensitivity: float32 [64, 128, 512], P('gx', 'gy', 'gz')
The draws below stay inside these ranges and needn't reach their ends.
All inputs are finite; a program needn't handle non-finite values.
Results may differ from the reference program's by a relative error of at most 0.0003.
Values sent between devices are 32-bit elements; how exact they have to be, the bound alone decides.
No kernel may reach another device: no remote copies, remote signals or barrier semaphores. Data moves between devices by JAX's collectives and lax.ppermute only.
A program may use at most 64 MiB of HBM per device.

```python
import math
import jax
import jax.numpy as jnp

ITERS = 6
NX = 64
NY = 128
NZ = 512


def face_ramp(length):
    width = max(1, min(16, length // 4))
    position = jnp.arange(length, dtype=jnp.float32)
    distance = jnp.minimum((float(length) - position) / float(width), 1.0)
    return jnp.sin(0.5 * math.pi * distance) ** 2


def draw_displacement(key, part):
    noise_key, sign_key = jax.random.split(jax.random.fold_in(key, 11))
    amplitude = 9.0
    noise = 0.6 * jnp.clip(jax.random.normal(noise_key, (3, NX, NY, NZ), jnp.float32), -6.0, 6.0)
    flip = jnp.where(jax.random.uniform(sign_key, (), jnp.float32) < 0.5, -1.0, 1.0)
    phase = 0.5 * math.pi * jnp.arange(NX, dtype=jnp.float32)
    envelope = face_ramp(NY)[:, None] * face_ramp(NZ)[None, :]
    along = amplitude * flip * jnp.sin(phase)[:, None, None] * envelope[None, :, :]
    across = amplitude * flip * 2.0 / math.sqrt(3.0) * jnp.cos(phase)[:, None, None] * envelope[None, :, :]
    smooth = jnp.stack([along, across, jnp.zeros((NX, NY, NZ), jnp.float32)], axis=0)
    return smooth + noise


def level_of(key, shape, cuts, low, high):
    level, own = 1.0, jax.random.fold_in(key, 6)
    for dim, blocks in cuts:
        steps = jnp.exp(jax.random.uniform(jax.random.fold_in(own, dim), (blocks,), jnp.float32, low / len(cuts), high / len(cuts)))
        level = level * jnp.repeat(steps, shape[dim] // blocks).reshape([-1 if axis == dim else 1 for axis in range(len(shape))])
    return level


def setup_inputs(seed: int = 0) -> dict:
    key_of = jax.random.split(jax.random.key(seed), 3)
    return {
        "displacement": draw_displacement(jax.random.fold_in(key_of[2], 71), 0),
        "density": jnp.clip(0.1 + 0.9 * jax.random.uniform(key_of[1], (NX, NY, NZ), jnp.float32) ** level_of(key_of[1], (NX, NY, NZ), ((0, 8), (1, 8), (2, 4)), -0.2, 0.2), 0.1, 1.0),
    }


lame_first = 0.3 / (1.3 * 0.4)
shear_modulus = 1.0 / 2.6
power_scale = 3.0
damping = 0.6
shift_term = 0.1
diag_factor = (lame_first + 3.0 * shear_modulus) / 16.0
CORNERS = [(first, second, third) for first in (0, 1) for second in (0, 1) for third in (0, 1)]
OFFSETS = [((first, second, third), 2.5 - math.sqrt(first * first + second * second + third * third)) for first in range(-2, 3) for second in range(-2, 3) for third in range(-2, 3) if first * first + second * second + third * third <= 4]

def window(array, anchor, extent):
    return array[:, anchor[0]:anchor[0] + extent[0], anchor[1]:anchor[1] + extent[1], anchor[2]:anchor[2] + extent[2]]

def window_cells(array, anchor, extent):
    return array[anchor[0]:anchor[0] + extent[0], anchor[1]:anchor[1] + extent[1], anchor[2]:anchor[2] + extent[2]]

def gradients(padded, offset, extent):
    totals = [0.0, 0.0, 0.0]
    for corner in CORNERS:
        piece = window(padded, (offset + corner[0], offset + corner[1], offset + corner[2]), extent)
        for direction in range(3):
            totals[direction] = totals[direction] + (2 * corner[direction] - 1) * piece
    return 0.25 * jnp.concatenate(totals, axis=0)

def strains(grad_all):
    return [grad_all[0], grad_all[4], grad_all[8], grad_all[3] + grad_all[1], grad_all[7] + grad_all[5], grad_all[2] + grad_all[6]]

def stiffen(values):
    trace = values[0] + values[1] + values[2]
    return [lame_first * trace + 2.0 * shear_modulus * values[0], lame_first * trace + 2.0 * shear_modulus * values[1], lame_first * trace + 2.0 * shear_modulus * values[2], shear_modulus * values[3], shear_modulus * values[4], shear_modulus * values[5]]

def spread(terms):
    return jnp.stack([terms[0], terms[3], terms[5], terms[3], terms[1], terms[4], terms[5], terms[4], terms[2]], axis=0)

def assemble(padded, extent):
    result = 0.0
    for corner in CORNERS:
        anchor = (1 - corner[0], 1 - corner[1], 1 - corner[2])
        for direction in range(3):
            piece = window(padded[3 * direction:3 * direction + 3], anchor, extent)
            result = result + 0.25 * (2 * corner[direction] - 1) * piece
    return result

def mises(sigma):
    return sigma[0] * sigma[0] + sigma[1] * sigma[1] + sigma[2] * sigma[2] - sigma[0] * sigma[1] - sigma[1] * sigma[2] - sigma[2] * sigma[0] + 3.0 * (sigma[3] * sigma[3] + sigma[4] * sigma[4] + sigma[5] * sigma[5])

def mises_slope(sigma):
    return [2.0 * sigma[0] - sigma[1] - sigma[2], 2.0 * sigma[1] - sigma[2] - sigma[0], 2.0 * sigma[2] - sigma[0] - sigma[1], 6.0 * sigma[3], 6.0 * sigma[4], 6.0 * sigma[5]]

def pad_nodes(field):
    return jnp.pad(field, ((0, 0), (1, 1), (1, 1), (1, 1)))

def reference(displacement, density):
    extent = density.shape
    base = stiffen(strains(gradients(pad_nodes(displacement), 1, extent)))
    rooted = jnp.sqrt(density)
    sigma = [rooted * value for value in base]
    stress = jnp.sqrt(mises(sigma) + 1.0)
    score = power_scale * stress
    top = jnp.max(score)
    total = jnp.sum(jnp.exp(score - top))
    aggregate = (top + jnp.log(total)) / power_scale
    weight = jnp.exp(score - top) / total * float(extent[0] * extent[1] * extent[2])
    factor = weight / (2.0 * stress)
    slope = [factor * value for value in mises_slope(sigma)]
    load = assemble(pad_nodes(spread(stiffen([rooted * value for value in slope]))), extent)
    stiff = 0.01 + 0.99 * density ** 3
    stiff_pad = jnp.pad(stiff, 2)
    summed = 0.0
    for corner in CORNERS:
        summed = summed + window_cells(stiff_pad, (2 - corner[0], 2 - corner[1], 2 - corner[2]), extent)
    diag = diag_factor * summed + shift_term

    def operate(field):
        values = stiffen(strains(gradients(pad_nodes(field), 1, extent)))
        return assemble(pad_nodes(spread([stiff * value for value in values])), extent) + shift_term * field
    adjoint = damping * load / diag
    for sweep in range(1, ITERS):
        adjoint = adjoint + damping * (load - operate(adjoint)) / diag
    other = strains(gradients(pad_nodes(adjoint), 1, extent))
    explicit = sum((slope[index] * base[index] for index in range(6))) / (2.0 * rooted)
    worked = sum((base[index] * other[index] for index in range(6)))
    raw = explicit - 2.97 * density * density * worked
    inside = jnp.pad(jnp.ones(extent, jnp.float32), 2)
    hsum = 0.0
    for offset, factor_w in OFFSETS:
        hsum = hsum + factor_w * window_cells(inside, (2 + offset[0], 2 + offset[1], 2 + offset[2]), extent)
    scaled = jnp.pad(raw / hsum, 2)
    sensitivity = 0.0
    for offset, factor_w in OFFSETS:
        sensitivity = sensitivity + factor_w * window_cells(scaled, (2 + offset[0], 2 + offset[1], 2 + offset[2]), extent)
    return (aggregate, adjoint, sensitivity)
```

```python
import functools
import math

import jax
import jax.numpy as jnp
from jax import lax
from jax.experimental import pallas as pl
from jax.experimental.pallas import tpu as pltpu
from jax.sharding import PartitionSpec as P

ITERS = 6
lame_first = 0.3 / (1.3 * 0.4)
shear_modulus = 1.0 / 2.6
lame_ratio = lame_first / shear_modulus
power_scale = 3.0
damping = 0.6
shift_term = 0.1
diag_factor = (lame_first + 3.0 * shear_modulus) / 16.0
W1, W2, W3 = (2.5 - math.sqrt(n) for n in (1, 2, 3))
W4 = 0.5
AXES = ("gx", "gy", "gz")

BX, BY, BZ = 8, 16, 128
NODES, CELLS = 25, 24
ROWS = 40
F32 = jnp.float32
VM = 24 * 1024 * 1024


def tile(value):
    return jax.ShapeDtypeStruct(value, F32)


def kernel_call(body, outs, name, scratch=(), flops=1_000_000, aliases=None):
    spec = pl.BlockSpec(memory_space=pltpu.VMEM)

    def run(*args):
        return pl.pallas_call(
            body,
            out_shape=[tile(shape) for shape in outs],
            in_specs=[spec] * len(args),
            out_specs=[spec] * len(outs),
            scratch_shapes=list(scratch),
            input_output_aliases=aliases or {},
            name=name,
            compiler_params=pltpu.CompilerParams(vmem_limit_bytes=VM),
            cost_estimate=pl.CostEstimate(flops=flops, bytes_accessed=1_000_000, transcendentals=0),
        )(*args)

    return run


def rolled(value, shift, axis):
    shift = shift % value.shape[axis]
    return value if shift == 0 else pltpu.roll(value, shift, axis)


def lanes():
    return lax.broadcasted_iota(jnp.int32, (8, 128), 1)


def rows():
    return lax.broadcasted_iota(jnp.int32, (8, 128), 0)


def split(value):
    return [value[8 * g : 8 * g + 8] for g in range(4)], value[32:40]


def join(main, strip):
    return jnp.concatenate([*main, strip], axis=0)


def z_next(value):
    main, strip = split(value)
    lane = lanes()
    moved = [rolled(m, -1, 1) for m in main]
    out = [jnp.where(lane == 127, rolled(strip, 127 - 32 * g, 1), moved[g]) for g in range(4)]
    tail = rolled(strip, -1, 1)
    for g in range(4):
        tail = jnp.where(lane == 32 * g + 31, rolled(moved[g], 32 * g + 32, 1), tail)
    return join(out, tail)


def z_prev(value):
    main, strip = split(value)
    lane = lanes()
    moved = [rolled(m, 1, 1) for m in main]
    out = [jnp.where(lane == 0, rolled(strip, 97 - 32 * g, 1), moved[g]) for g in range(4)]
    tail = rolled(strip, 1, 1)
    for g in range(4):
        tail = jnp.where(lane == 32 * g, rolled(moved[g], 32 * g, 1), tail)
    return join(out, tail)


def y_next(value, beyond=None):
    main, strip = split(value)
    row = rows()
    turned = [rolled(m, -1, 0) for m in main]
    follow = [turned[1], turned[2], turned[3], turned[3] if beyond is None else beyond[0]]
    out = [jnp.where(row == 7, follow[g], turned[g]) for g in range(4)]
    tail = rolled(strip, -1, 0)
    after = rolled(tail, -32, 1)
    if beyond is not None:
        after = jnp.where(lanes() >= 96, beyond[1], after)
    return join(out, jnp.where(row == 7, after, tail))


def y_prev(value):
    main, strip = split(value)
    row = rows()
    turned = [rolled(m, 1, 0) for m in main]
    before = [turned[0], turned[0], turned[1], turned[2]]
    out = [jnp.where(row == 0, before[g], turned[g]) for g in range(4)]
    tail = rolled(strip, 1, 0)
    return join(out, jnp.where(row == 0, rolled(tail, 32, 1), tail))


def pack_z(disp, dens, up, down):
    lane = lanes()
    for c in range(4):
        for k in range(4):
            top = bottom = jnp.zeros((8, 128), F32)
            for q in range(4):
                x, t = k + 4 * (q // 2), 8 * (q % 2)
                value = disp[c, x, t : t + 8, :] if c < 3 else dens[x, t : t + 8, :]
                mine = (lane >= 32 * q) & (lane < 32 * q + 32)
                top = jnp.where(mine & (lane >= 32 * q + 24), rolled(value, 32 * q + 32, 1), top)
                bottom = jnp.where(mine & (lane < 32 * q + 9), rolled(value, 32 * q, 1), bottom)
            up[4 * c + k] = top
            down[4 * c + k] = bottom


def pack_y(mid, low, high, far, up, down):
    lane = lanes()
    odd = (lane // 32) % 2 == 1
    sources = (low, mid, high)
    for s, src in enumerate(sources):
        for i in range(32):
            up[32 * s + i] = src[2 * i + 1]
            down[32 * s + i] = src[2 * i]
        for c in range(4):
            for k in range(2):
                first, second = src[64 + 4 * c + k], src[64 + 4 * c + k + 2]
                up[99 + 8 * s + 2 * c + k] = jnp.where(odd, first, rolled(second, -32, 1))
                down[99 + 8 * s + 2 * c + k] = jnp.where(odd, rolled(second, 32, 1), first)
        for i in range(24):
            r = 24 * s + i
            down[126 + r // 8, r % 8 : r % 8 + 1, :] = src[2 * i + 1, 0:1, :]
        for i in range(12):
            r = 12 * s + i
            down[136 + r // 8, r % 8 : r % 8 + 1, :] = src[64 + i, 0:1, :]
    for c in range(3):
        up[96 + c] = far[2 * c + 1]
        down[96 + c] = far[2 * c]
        up[123 + c] = far[6 + c]
        down[123 + c] = far[6 + c]
        r = 72 + c
        down[126 + r // 8, r % 8 : r % 8 + 1, :] = far[2 * c + 1, 0:1, :]
        r = 36 + c
        down[136 + r // 8, r % 8 : r % 8 + 1, :] = far[6 + c, 0:1, :]


def unpacked(c, p, sources, far, below, above):
    lane = lanes()
    group = lane // 32
    if p < 24:
        s, x = divmod(p, 8)
        src, i, k = sources[s], 8 * c + x, x % 4
        own = rolled(src[64 + 4 * c + k], 32 if x < 4 else -32, 1)
        slot = 99 + 8 * s + 2 * c + x % 2
        under = rolled(below[slot], {0: -32, 1: -96, 2: 0, 3: -64}[(1 if x >= 4 else 0) + (2 if k >= 2 else 0)], 1)
        over = rolled(above[slot], {0: 96, 1: 32, 2: 64, 3: 0}[(1 if x >= 4 else 0) + (2 if k >= 2 else 0)], 1)
        main = [below[32 * s + i], src[2 * i], src[2 * i + 1], above[32 * s + i]]
        r, q = 24 * s + i, 12 * s + 4 * c + k
        turn = 64 if x < 4 else 0
    else:
        own = rolled(far[6 + c], 32, 1)
        under = rolled(below[123 + c], -32, 1)
        over = rolled(above[123 + c], 96, 1)
        main = [below[96 + c], far[2 * c], far[2 * c + 1], above[96 + c]]
        r, q, turn = 72 + c, 36 + c, 64
    strip = jnp.where(group == 0, under, jnp.where(group == 3, over, own))
    if c == 3:
        return join(main, strip), None
    line = jnp.broadcast_to(above[126 + r // 8, r % 8 : r % 8 + 1, :], (8, 128))
    edge = jnp.broadcast_to(above[136 + q // 8, q % 8 : q % 8 + 1, :], (8, 128))
    return join(main, strip), (line, rolled(edge, turn, 1))


def corner_sums(value, beyond=None):
    if beyond is not None:
        following = y_next(value, beyond)
        both, change = following + value, following - value
        first, second = z_next(both), z_next(change)
        return first + both, second + change, first - both
    following = z_next(value)
    both, change = following + value, following - value
    after = y_next(both)
    return after + both, after - both, y_next(change) + change


def strain_of(new, old):
    grad = [[new[c][0] - old[c][0] for c in range(3)]]
    grad.append([new[c][1] + old[c][1] for c in range(3)])
    grad.append([new[c][2] + old[c][2] for c in range(3)])
    return [
        grad[0][0],
        grad[1][1],
        grad[2][2],
        grad[0][1] + grad[1][0],
        grad[1][2] + grad[2][1],
        grad[2][0] + grad[0][2],
    ]


def scaled_stress(values, factor):
    trace = lame_ratio * (values[0] + values[1] + values[2])
    return [factor * (trace + 2.0 * v) for v in values[:3]] + [factor * v for v in values[3:]]


def forces(prev, here):
    add = [prev[i] + here[i] for i in range(6)]
    sub = {i: prev[i] - here[i] for i in (0, 3, 5)}
    out = []
    for along_x, along_y, along_z in ((0, 3, 5), (3, 1, 4), (5, 4, 2)):
        a, b, w = sub[along_x], add[along_y], add[along_z]
        first = y_prev(a + b) + (a - b)
        second = y_prev(w) + w
        out.append(z_prev(first + second) + (first - second))
    return out


def get3(ref, p):
    return [ref[c, p] for c in range(3)]


def put_corners(ref, values):
    for c in range(3):
        for i in range(3):
            ref[3 * c + i] = values[c][i]


def get_corners(ref):
    return [[ref[3 * c + i] for i in range(3)] for c in range(3)]


def mises(v):
    return (
        v[0] * v[0] + v[1] * v[1] + v[2] * v[2] - v[0] * v[1] - v[1] * v[2] - v[2] * v[0]
        + 3.0 * (v[3] * v[3] + v[4] * v[4] + v[5] * v[5])
    )


def mises_slope(v):
    return [
        2.0 * v[0] - v[1] - v[2],
        2.0 * v[1] - v[2] - v[0],
        2.0 * v[2] - v[0] - v[1],
        6.0 * v[3],
        6.0 * v[4],
        6.0 * v[5],
    ]


def stress_kernel(mid, low, high, far, below, above, base, cells, stress, stats, disp, line, edge, corners):
    sources = (low, mid, high)
    for p in range(NODES):
        for c in range(4 if p < CELLS else 3):
            value, beyond = unpacked(c, p, sources, far, below, above)
            if c == 3:
                cells[p] = value
            else:
                disp[c, p] = value
                line[c, p] = beyond[0]
                edge[c, p] = beyond[1]

    def planes(p):
        return [corner_sums(disp[c, p], (line[c, p], edge[c, p])) for c in range(3)]

    put_corners(corners, planes(0))

    def step(p, most):
        new = planes(p + 1)
        values = scaled_stress(strain_of(new, get_corners(corners)), 0.25 * shear_modulus)
        put_corners(corners, new)
        dens = cells[p]
        for i in range(6):
            base[i, p] = values[i]
        local = jnp.sqrt(dens * mises(values) + 1.0)
        stress[p] = local
        return jnp.maximum(most, jnp.where(dens > 0.0, local, 0.0))

    most = lax.fori_loop(0, CELLS, step, jnp.zeros((ROWS, 128), F32))
    top = power_scale * jnp.max(most, axis=(0, 1), keepdims=True)

    def add(p, total):
        return total + jnp.exp(power_scale * stress[p, 8:24, :] - top)

    total = lax.fori_loop(8, 16, add, jnp.zeros((BY, 128), F32))
    total = jnp.sum(total, axis=(0, 1), keepdims=True)
    stats[0] = jnp.broadcast_to(top, (8, 128))
    stats[1] = jnp.broadcast_to(total, (8, 128))


def load_kernel(base, cells, stress, stats, rhs, stiff, weight, explicit, field, held, kept):
    top = stats[0, 0:1, 0:1]

    def element(p):
        dens = cells[p]
        values = [base[i, p] for i in range(6)]
        local = stress[p]
        factor = jnp.where(dens > 0.0, jnp.exp(power_scale * local - top), 0.0) / (2.0 * local)
        explicit[p] = factor * mises(values)
        part = scaled_stress(mises_slope(values), (0.25 * shear_modulus) * dens * factor)
        rigid = jnp.where(dens > 0.0, 0.01 + 0.99 * (dens * dens * dens), 0.0)
        stiff[p] = (shear_modulus / 16.0) * rigid
        return part, rigid

    part, rigid = element(0)
    for i in range(6):
        held[i] = part[i]
    kept[...] = rigid

    def step(p, carry):
        part, rigid = element(p)
        load = forces([held[i] for i in range(6)], part)
        for i in range(6):
            held[i] = part[i]
        total = kept[...] + rigid
        kept[...] = rigid
        total = total + y_prev(total)
        total = total + z_prev(total)
        own = jnp.where(cells[p] > 0.0, damping / (diag_factor * total + shift_term), 0.0)
        weight[p] = own
        for c in range(3):
            value = own * load[c]
            rhs[c, p] = value
            field[c, p] = value
        return carry

    lax.fori_loop(1, CELLS, step, 0)


def sweep_into(field, rhs, stiff, weight, held, corners, lo, hi):
    def planes(p):
        return [corner_sums(v) for v in get3(field, p)]

    def element(new, old, p):
        return scaled_stress(strain_of(new, old), stiff[p])

    first, second = planes(lo - 1), planes(lo)
    part = element(second, first, lo - 1)
    for i in range(6):
        held[i] = part[i]
    put_corners(corners, second)

    def step(p, carry):
        new = planes(p + 1)
        part = element(new, get_corners(corners), p)
        put_corners(corners, new)
        force = forces([held[i] for i in range(6)], part)
        for i in range(6):
            held[i] = part[i]
        own = weight[p]
        keep = 1.0 - shift_term * own
        for c in range(3):
            field[c, p] = keep * field[c, p] + rhs[c, p] - own * force[c]
        return carry

    lax.fori_loop(lo, hi + 1, step, 0)


def positions(axis, length, cell):
    whole = lax.axis_size(axis) * length
    place = lax.axis_index(axis) * length + cell
    return lambda o: ((place + o >= 0) & (place + o < whole)).astype(F32)


def sweeps_kernel(rhs, stiff, weight, explicit, base, cells, start, adjoint, sens, field, held, corners, near, side, out):
    for c in range(3):
        for p in range(1, CELLS):
            field[c, p] = start[c, p]
    for k in range(1, ITERS):
        sweep_into(field, rhs, stiff, weight, held, corners, 1 + k, 23 - k)
    final_part(field, explicit, base, cells, adjoint, sens, corners, near, side, out)


def final_part(field, explicit, base, cells, adjoint, sens, corners, near, side, out):
    for c in range(3):
        adjoint[c] = field[c, 8:16, 8:24, :]

    row = lax.broadcasted_iota(jnp.int32, (ROWS, 128), 0)
    lane = lax.broadcasted_iota(jnp.int32, (ROWS, 128), 1)
    group, place = lane // 32, lane % 32
    main = row < 32
    y_cell = jnp.where(main, row - 8, 8 * group + row - 40)
    z_cell = jnp.where(main, lane, jnp.where(place < 16, 128 + place, place - 32))
    in_y, in_z = positions("gy", BY, y_cell), positions("gz", BZ, z_cell)
    ys, zs = {o: in_y(o) for o in range(-2, 3)}, {o: in_z(o) for o in range(-2, 3)}
    beside = ys[-1] + ys[1]
    across = zs[-1] + zs[1]
    ones = beside * zs[0] + ys[0] * across
    diagonal = beside * across
    twos = (ys[-2] + ys[2]) * zs[0] + ys[0] * (zs[-2] + zs[2])
    centre = ys[0] * zs[0]
    near_0 = 2.5 * centre + W1 * ones + W2 * diagonal + W4 * twos
    near_1 = W1 * centre + W2 * ones + W3 * diagonal
    near_2 = W4 * centre

    def planes(p):
        return [corner_sums(v) for v in get3(field, p)]

    put_corners(corners, planes(6))

    def step(p, carry):
        new = planes(p + 1)
        strain = strain_of(new, get_corners(corners))
        put_corners(corners, new)
        dens = cells[p]
        worked = base[0, p] * strain[0]
        for i in range(1, 6):
            worked = worked + base[i, p] * strain[i]
        raw = explicit[p] - (0.25 * 2.97) * dens * dens * worked
        in_x = positions("gx", BX, p - 8)
        hsum = near_0 + near_1 * (in_x(-1) + in_x(1)) + near_2 * (in_x(-2) + in_x(2))
        value = jnp.where(dens > 0.0, raw / jnp.where(dens > 0.0, hsum, 1.0), 0.0)
        above, under = z_next(value), z_prev(value)
        left, right = y_next(value), y_prev(value)
        row_pair = above + under
        unit = row_pair + (left + right)
        corner = y_next(row_pair) + y_prev(row_pair)
        two = z_next(above) + z_prev(under) + y_next(left) + y_prev(right)
        near[p - 6] = (2.5 * value + W1 * unit + W2 * corner + W4 * two)[8:24]
        side[p - 6] = (W1 * value + W2 * unit + W3 * corner)[8:24]
        out[p - 6] = (W4 * value)[8:24]
        return carry

    lax.fori_loop(6, 18, step, 0)
    for p in range(8):
        q = p + 2
        sens[p] = near[q] + (side[q - 1] + side[q + 1]) + (out[q - 2] + out[q + 2])


def passed(block, axis, distance):
    count = lax.axis_size(axis)
    return lax.ppermute(block, axis, [(i, i + distance) for i in range(count) if 0 <= i + distance < count])


def merged(mine, other):
    larger = jnp.maximum(mine[0], other[0])
    gap = jnp.exp(jnp.minimum(mine[0], other[0]) - larger)
    first = mine[0] >= other[0]
    total = jnp.where(first, mine[1], other[1]) + jnp.where(first, other[1], mine[1]) * gap
    return jnp.stack([larger, total])


def on_device(displacement, density):
    plane = (ROWS, 128)
    up, down = kernel_call(pack_z, [(16, 8, 128)] * 2, "pack_z")(displacement, density)
    below_z, above_z = passed(up, "gz", 1), passed(down, "gz", -1)
    mid = jnp.concatenate(
        [displacement.reshape(48, 8, 128), density.reshape(16, 8, 128), below_z + above_z], axis=0
    )
    far = jnp.concatenate([mid[t : t + n] for t, n in ((0, 2), (16, 2), (32, 2), (64, 1), (68, 1), (72, 1))], axis=0)
    low, high, far = passed(mid, "gx", 1), passed(mid, "gx", -1), passed(far, "gx", -2)
    up, down = kernel_call(pack_y, [(126, 8, 128), (141, 8, 128)], "pack_y")(mid, low, high, far)
    below, above = passed(up, "gy", 1), passed(down, "gy", -1)
    base, cells, stress, stats = kernel_call(
        stress_kernel,
        [(6, CELLS, *plane), (CELLS, *plane), (CELLS, *plane), (2, 8, 128)],
        "stress",
        [
            pltpu.VMEM((3, NODES, *plane), F32),
            pltpu.VMEM((3, NODES, 8, 128), F32),
            pltpu.VMEM((3, NODES, 8, 128), F32),
            pltpu.VMEM((9, *plane), F32),
        ],
    )(mid, low, high, far, below, above)
    own_top = stats[0, 0, 0]
    everyone = stats
    for axis in AXES:
        count, hop = lax.axis_size(axis), 1
        while hop < count:
            other = lax.ppermute(everyone, axis, [(i, i ^ hop) for i in range(count)])
            everyone = merged(everyone, other)
            hop *= 2
    rhs, stiff, weight, explicit, field = kernel_call(
        load_kernel,
        [(3, CELLS, *plane), (CELLS, *plane), (CELLS, *plane), (CELLS, *plane), (3, CELLS, *plane)],
        "load",
        [pltpu.VMEM((6, *plane), F32), pltpu.VMEM(plane, F32)],
    )(base, cells, stress, stats)
    adjoint, sens = kernel_call(
        sweeps_kernel,
        [(3, BX, BY, BZ), (BX, BY, BZ)],
        "sweeps",
        [
            pltpu.VMEM((3, CELLS, *plane), F32),
            pltpu.VMEM((6, *plane), F32),
            pltpu.VMEM((9, *plane), F32),
            pltpu.VMEM((12, BY, 128), F32),
            pltpu.VMEM((12, BY, 128), F32),
            pltpu.VMEM((12, BY, 128), F32),
        ],
    )(rhs, stiff, weight, explicit, base, cells, field)
    top, total = everyone[0, 0, 0], everyone[1, 0, 0]
    elements = BX * BY * BZ * lax.axis_size("gx") * lax.axis_size("gy") * lax.axis_size("gz")
    scale = jnp.exp(own_top - top) / total * float(elements)
    aggregate = (top + jnp.log(total)) / power_scale
    return aggregate, scale * adjoint, scale * sens


def solution(mesh):
    placed = (P(None, "gx", "gy", "gz"), P("gx", "gy", "gz"))
    return jax.shard_map(
        on_device,
        mesh=mesh,
        in_specs=placed,
        out_specs=(P(), P(None, "gx", "gy", "gz"), P("gx", "gy", "gz")),
        check_vma=False,
    )
```

```python
import functools
import math

import jax
import jax.numpy as jnp
from jax import lax
from jax.experimental import pallas as pl
from jax.experimental.pallas import tpu as pltpu
from jax.sharding import PartitionSpec as P

ITERS = 6
lame_first = 0.3 / (1.3 * 0.4)
shear_modulus = 1.0 / 2.6
lame_ratio = lame_first / shear_modulus
power_scale = 3.0
damping = 0.6
shift_term = 0.1
diag_factor = (lame_first + 3.0 * shear_modulus) / 16.0
W1, W2, W3 = (2.5 - math.sqrt(n) for n in (1, 2, 3))
W4 = 0.5
AXES = ("gx", "gy", "gz")

BX, BY, BZ = 8, 16, 128
NODES, CELLS = 25, 24
ROWS = 40
F32 = jnp.float32
VM = 24 * 1024 * 1024
GROUP = 3
BUSY = 20_000_000


def tile(value):
    return jax.ShapeDtypeStruct(value, F32)


def kernel_call(body, outs, name, scratch=(), flops=1_000_000, aliases=None):
    spec = pl.BlockSpec(memory_space=pltpu.VMEM)

    def run(*args):
        return pl.pallas_call(
            body,
            out_shape=[tile(shape) for shape in outs],
            in_specs=[spec] * len(args),
            out_specs=[spec] * len(outs),
            scratch_shapes=list(scratch),
            input_output_aliases=aliases or {},
            name=name,
            compiler_params=pltpu.CompilerParams(vmem_limit_bytes=VM),
            cost_estimate=pl.CostEstimate(flops=flops, bytes_accessed=1_000_000, transcendentals=0),
        )(*args)

    return run


def rolled(value, shift, axis):
    shift = shift % value.shape[axis]
    return value if shift == 0 else pltpu.roll(value, shift, axis)


def lanes():
    return lax.broadcasted_iota(jnp.int32, (8, 128), 1)


def rows():
    return lax.broadcasted_iota(jnp.int32, (8, 128), 0)


def split(value):
    return [value[8 * g : 8 * g + 8] for g in range(4)], value[32:40]


def join(main, strip):
    return jnp.concatenate([*main, strip], axis=0)


def z_next(value):
    main, strip = split(value)
    lane = lanes()
    moved = [rolled(m, -1, 1) for m in main]
    out = [jnp.where(lane == 127, rolled(strip, 127 - 32 * g, 1), moved[g]) for g in range(4)]
    tail = rolled(strip, -1, 1)
    for g in range(4):
        tail = jnp.where(lane == 32 * g + 31, rolled(main[g], 32 * g + 31, 1), tail)
    return join(out, tail)


def z_prev(value):
    main, strip = split(value)
    lane = lanes()
    moved = [rolled(m, 1, 1) for m in main]
    out = [jnp.where(lane == 0, rolled(strip, 97 - 32 * g, 1), moved[g]) for g in range(4)]
    tail = rolled(strip, 1, 1)
    for g in range(4):
        tail = jnp.where(lane == 32 * g, rolled(main[g], 32 * g + 1, 1), tail)
    return join(out, tail)


def y_next(value, beyond=None):
    main, strip = split(value)
    row = rows()
    turned = [rolled(m, -1, 0) for m in main]
    follow = [turned[1], turned[2], turned[3], turned[3] if beyond is None else beyond[0]]
    out = [jnp.where(row == 7, follow[g], turned[g]) for g in range(4)]
    tail = rolled(strip, -1, 0)
    after = rolled(tail, -32, 1)
    if beyond is not None:
        after = jnp.where(lanes() >= 96, beyond[1], after)
    return join(out, jnp.where(row == 7, after, tail))


def y_prev(value):
    main, strip = split(value)
    row = rows()
    turned = [rolled(m, 1, 0) for m in main]
    before = [turned[0], turned[0], turned[1], turned[2]]
    out = [jnp.where(row == 0, before[g], turned[g]) for g in range(4)]
    tail = rolled(strip, 1, 0)
    return join(out, jnp.where(row == 0, rolled(tail, 32, 1), tail))


def pack_z(disp, dens, up, down):
    lane = lanes()
    for c in range(4):
        for k in range(4):
            top = bottom = jnp.zeros((8, 128), F32)
            for q in range(4):
                x, t = k + 4 * (q // 2), 8 * (q % 2)
                value = disp[c, x, t : t + 8, :] if c < 3 else dens[x, t : t + 8, :]
                mine = (lane >= 32 * q) & (lane < 32 * q + 32)
                top = jnp.where(mine & (lane >= 32 * q + 24), rolled(value, 32 * q + 32, 1), top)
                bottom = jnp.where(mine & (lane < 32 * q + 9), rolled(value, 32 * q, 1), bottom)
            up[4 * c + k] = top
            down[4 * c + k] = bottom


def pack_y(mid, low, high, far, up, down):
    lane = lanes()
    odd = (lane // 32) % 2 == 1
    sources = (low, mid, high)
    for s, src in enumerate(sources):
        for i in range(32):
            up[32 * s + i] = src[2 * i + 1]
            down[32 * s + i] = src[2 * i]
        for c in range(4):
            for k in range(2):
                first, second = src[64 + 4 * c + k], src[64 + 4 * c + k + 2]
                up[99 + 8 * s + 2 * c + k] = jnp.where(odd, first, rolled(second, -32, 1))
                down[99 + 8 * s + 2 * c + k] = jnp.where(odd, rolled(second, 32, 1), first)
        for i in range(24):
            r = 24 * s + i
            down[126 + r // 8, r % 8 : r % 8 + 1, :] = src[2 * i + 1, 0:1, :]
        for i in range(12):
            r = 12 * s + i
            down[136 + r // 8, r % 8 : r % 8 + 1, :] = src[64 + i, 0:1, :]
    for c in range(3):
        up[96 + c] = far[2 * c + 1]
        down[96 + c] = far[2 * c]
        up[123 + c] = far[6 + c]
        down[123 + c] = far[6 + c]
        r = 72 + c
        down[126 + r // 8, r % 8 : r % 8 + 1, :] = far[2 * c + 1, 0:1, :]
        r = 36 + c
        down[136 + r // 8, r % 8 : r % 8 + 1, :] = far[6 + c, 0:1, :]


def unpacked(c, p, sources, far, below, above):
    lane = lanes()
    group = lane // 32
    if p < 24:
        s, x = divmod(p, 8)
        src, i, k = sources[s], 8 * c + x, x % 4
        own = rolled(src[64 + 4 * c + k], 32 if x < 4 else -32, 1)
        slot = 99 + 8 * s + 2 * c + x % 2
        under = rolled(below[slot], {0: -32, 1: -96, 2: 0, 3: -64}[(1 if x >= 4 else 0) + (2 if k >= 2 else 0)], 1)
        over = rolled(above[slot], {0: 96, 1: 32, 2: 64, 3: 0}[(1 if x >= 4 else 0) + (2 if k >= 2 else 0)], 1)
        main = [below[32 * s + i], src[2 * i], src[2 * i + 1], above[32 * s + i]]
        r, q = 24 * s + i, 12 * s + 4 * c + k
        turn = 64 if x < 4 else 0
    else:
        own = rolled(far[6 + c], 32, 1)
        under = rolled(below[123 + c], -32, 1)
        over = rolled(above[123 + c], 96, 1)
        main = [below[96 + c], far[2 * c], far[2 * c + 1], above[96 + c]]
        r, q, turn = 72 + c, 36 + c, 64
    strip = jnp.where(group == 0, under, jnp.where(group == 3, over, own))
    if c == 3:
        return join(main, strip), None
    line = jnp.broadcast_to(above[126 + r // 8, r % 8 : r % 8 + 1, :], (8, 128))
    edge = jnp.broadcast_to(above[136 + q // 8, q % 8 : q % 8 + 1, :], (8, 128))
    return join(main, strip), (line, rolled(edge, turn, 1))


def corner_sums(value, beyond=None):
    if beyond is not None:
        following = y_next(value, beyond)
        both, change = following + value, following - value
        first, second = z_next(both), z_next(change)
        return first + both, second + change, first - both
    following = z_next(value)
    both, change = following + value, following - value
    after = y_next(both)
    return after + both, after - both, y_next(change) + change


def strain_of(new, old):
    grad = [[new[c][0] - old[c][0] for c in range(3)]]
    grad.append([new[c][1] + old[c][1] for c in range(3)])
    grad.append([new[c][2] + old[c][2] for c in range(3)])
    return [
        grad[0][0],
        grad[1][1],
        grad[2][2],
        grad[0][1] + grad[1][0],
        grad[1][2] + grad[2][1],
        grad[2][0] + grad[0][2],
    ]


def scaled_stress(values, factor):
    trace = lame_ratio * (values[0] + values[1] + values[2])
    return [factor * (trace + 2.0 * v) for v in values[:3]] + [factor * v for v in values[3:]]


def forces(prev, here):
    add = [prev[i] + here[i] for i in range(6)]
    sub = {i: prev[i] - here[i] for i in (0, 3, 5)}
    out = []
    for along_x, along_y, along_z in ((0, 3, 5), (3, 1, 4), (5, 4, 2)):
        a, b, w = sub[along_x], add[along_y], add[along_z]
        first = y_prev(a + b) + (a - b)
        second = y_prev(w) + w
        out.append(z_prev(first + second) + (first - second))
    return out


def get3(ref, p):
    return [ref[c, p] for c in range(3)]


def put_corners(ref, values):
    for c in range(3):
        for i in range(3):
            ref[3 * c + i] = values[c][i]


def get_corners(ref):
    return [[ref[3 * c + i] for i in range(3)] for c in range(3)]


def mises(v):
    return (
        v[0] * v[0] + v[1] * v[1] + v[2] * v[2] - v[0] * v[1] - v[1] * v[2] - v[2] * v[0]
        + 3.0 * (v[3] * v[3] + v[4] * v[4] + v[5] * v[5])
    )


def mises_slope(v):
    return [
        2.0 * v[0] - v[1] - v[2],
        2.0 * v[1] - v[2] - v[0],
        2.0 * v[2] - v[0] - v[1],
        6.0 * v[3],
        6.0 * v[4],
        6.0 * v[5],
    ]


def in_groups(lo, hi, size, body):
    full = (hi - lo) // size

    def step(i, carry):
        body(lo + size * i, size)
        return carry

    if full:
        lax.fori_loop(0, full, step, 0)
    if lo + size * full < hi:
        body(lo + size * full, hi - lo - size * full)


def own_kernel(mid, high, above, below, stats):
    lane = lanes()
    row = rows()

    def node(c, x):
        src, i, k = (mid, 8 * c + x, x % 4) if x < 8 else (high, 8 * c, 0)
        s = 1 if x < 8 else 2
        x = x % 8
        strip = src[64 + 4 * c + k]
        base = 64 if x >= 4 else 0
        far_strip = above[99 + 8 * s + 2 * c + x % 2]
        at = 64 * (x // 4) + (32 if k >= 2 else 0)
        main = [src[2 * i], src[2 * i + 1], above[32 * s + i]]
        edge = [rolled(strip, 127 - base, 1), rolled(strip, 95 - base, 1), rolled(far_strip, 127 - at, 1)]
        after = [jnp.where(lane == 127, edge[t], rolled(main[t], -1, 1)) for t in range(3)]
        both = [after[t] + main[t] for t in range(3)]
        change = [after[t] - main[t] for t in range(3)]

        def follow(v):
            turned = [rolled(t, -1, 0) for t in v]
            return [jnp.where(row == 7, turned[t + 1], turned[t]) for t in range(2)]

        both_next, change_next = follow(both), follow(change)
        join2 = lambda v: jnp.concatenate(v[:2], axis=0)
        both, change, both_next, change_next = join2(both), join2(change), join2(both_next), join2(change_next)
        return both_next + both, both_next - both, change_next + change

    scores = []
    old = [node(c, 0) for c in range(3)]
    for x in range(8):
        new = [node(c, x + 1) for c in range(3)]
        values = scaled_stress(strain_of(new, old), 0.25 * shear_modulus)
        old = new
        dens = mid[48 + 2 * x : 50 + 2 * x].reshape(BY, 128)
        scores.append(power_scale * jnp.sqrt(dens * mises(values) + 1.0))
    most = functools.reduce(jnp.maximum, scores)
    top = jnp.max(most, axis=(0, 1), keepdims=True)
    total = sum(jnp.exp(score - top) for score in scores)
    total = jnp.sum(total, axis=(0, 1), keepdims=True)
    stats[0] = jnp.broadcast_to(top, (8, 128))
    stats[1] = jnp.broadcast_to(total, (8, 128))


def beside(body, ins, outs):
    def run(*refs):
        refs[ins + 1 + outs][...] = refs[ins][...]
        body(*refs[:ins], *refs[ins + 1 : ins + 1 + outs], *refs[ins + 2 + outs :])

    return run


def widen_kernel(mid, low, high, far, below, above, disp, line, edge, cells):
    sources = (low, mid, high)
    for p in range(NODES):
        for c in range(4 if p < CELLS else 3):
            value, beyond = unpacked(c, p, sources, far, below, above)
            if c == 3:
                cells[p] = value
            else:
                disp[c, p] = value
                line[c, p] = beyond[0]
                edge[c, p] = beyond[1]


def stress_kernel(disp, line, edge, cells, base, stress, highest, corners):
    def planes(p):
        return [corner_sums(disp[c, p], (line[c, p], edge[c, p])) for c in range(3)]

    put_corners(corners, planes(0))
    highest[...] = jnp.zeros((ROWS, 128), F32)

    def step(p, n):
        news = [get_corners(corners)] + [planes(p + 1 + j) for j in range(n)]
        most = highest[...]
        for j in range(n):
            values = scaled_stress(strain_of(news[j + 1], news[j]), 0.25 * shear_modulus)
            dens = cells[p + j]
            for i in range(6):
                base[i, p + j] = values[i]
            local = jnp.sqrt(dens * mises(values) + 1.0)
            stress[p + j] = local
            most = jnp.maximum(most, jnp.where(dens > 0.0, local, 0.0))
        highest[...] = most
        put_corners(corners, news[n])

    in_groups(0, CELLS, GROUP, step)


def load_kernel(base, cells, stress, highest, rhs, stiff, weight, explicit, field, reference, held, kept):
    top = power_scale * jnp.max(highest[...], axis=(0, 1), keepdims=True)
    reference[...] = jnp.broadcast_to(top, (8, 128))

    def element(p):
        dens = cells[p]
        values = [base[i, p] for i in range(6)]
        local = stress[p]
        factor = jnp.where(dens > 0.0, jnp.exp(power_scale * local - top), 0.0) / (2.0 * local)
        explicit[p] = factor * mises(values)
        part = scaled_stress(mises_slope(values), (0.25 * shear_modulus) * dens * factor)
        rigid = jnp.where(dens > 0.0, 0.01 + 0.99 * (dens * dens * dens), 0.0)
        stiff[p] = (shear_modulus / 16.0) * rigid
        return part, rigid

    part, rigid = element(0)
    for i in range(6):
        held[i] = part[i]
    kept[...] = rigid
    for c in range(3):
        field[c, 0] = jnp.zeros((ROWS, 128), F32)
        field[c, CELLS] = jnp.zeros((ROWS, 128), F32)

    def step(p, n):
        parts = [([held[i] for i in range(6)], kept[...])] + [element(p + j) for j in range(n)]
        for i in range(6):
            held[i] = parts[n][0][i]
        kept[...] = parts[n][1]
        for j in range(n):
            load = forces(parts[j][0], parts[j + 1][0])
            total = parts[j][1] + parts[j + 1][1]
            total = total + y_prev(total)
            total = total + z_prev(total)
            own = jnp.where(cells[p + j] > 0.0, damping / (diag_factor * total + shift_term), 0.0)
            weight[p + j] = own
            for c in range(3):
                value = own * load[c]
                rhs[c, p + j] = value
                field[c, p + j] = value

    in_groups(1, CELLS, GROUP, step)


def sweep_kernel(lo, hi, start, rhs, stiff, weight, field, held, corners):
    def planes(p):
        return [corner_sums(v) for v in get3(start, p)]

    def element(new, old, p):
        return scaled_stress(strain_of(new, old), stiff[p])

    first, second = planes(lo - 1), planes(lo)
    part = element(second, first, lo - 1)
    for i in range(6):
        held[i] = part[i]
    put_corners(corners, second)

    def step(p, n):
        news = [get_corners(corners)] + [planes(p + 1 + j) for j in range(n)]
        put_corners(corners, news[n])
        part = [held[i] for i in range(6)]
        for j in range(n):
            here = element(news[j + 1], news[j], p + j)
            force = forces(part, here)
            part = here
            own = weight[p + j]
            keep = 1.0 - shift_term * own
            for c in range(3):
                field[c, p + j] = keep * start[c, p + j] + rhs[c, p + j] - own * force[c]
        for i in range(6):
            held[i] = part[i]

    count = -(-(hi + 1 - lo) // GROUP) * GROUP
    in_groups(lo, lo + count, GROUP, step)


def positions(axis, length, cell):
    whole = lax.axis_size(axis) * length
    place = lax.axis_index(axis) * length + cell
    return lambda o: ((place + o >= 0) & (place + o < whole)).astype(F32)


def final_kernel(field, explicit, base, cells, reference, everyone, adjoint, sens, aggregate, corners, near, side, out):
    elements = BX * BY * BZ * lax.axis_size("gx") * lax.axis_size("gy") * lax.axis_size("gz")
    top, total = everyone[0], everyone[1]
    scale = jnp.exp(reference[...] - top) / total * float(elements)
    aggregate[...] = (top + jnp.log(total)) / power_scale
    scale = jnp.broadcast_to(scale[0:1, 0:1], (BY, 128))
    for c in range(3):
        for p in range(8):
            adjoint[c, p] = scale * field[c, 8 + p, 8:24, :]

    row = lax.broadcasted_iota(jnp.int32, (ROWS, 128), 0)
    lane = lax.broadcasted_iota(jnp.int32, (ROWS, 128), 1)
    group, place = lane // 32, lane % 32
    main = row < 32
    y_cell = jnp.where(main, row - 8, 8 * group + row - 40)
    z_cell = jnp.where(main, lane, jnp.where(place < 16, 128 + place, place - 32))
    in_y, in_z = positions("gy", BY, y_cell), positions("gz", BZ, z_cell)
    ys, zs = {o: in_y(o) for o in range(-2, 3)}, {o: in_z(o) for o in range(-2, 3)}
    beside = ys[-1] + ys[1]
    across = zs[-1] + zs[1]
    ones = beside * zs[0] + ys[0] * across
    diagonal = beside * across
    twos = (ys[-2] + ys[2]) * zs[0] + ys[0] * (zs[-2] + zs[2])
    centre = ys[0] * zs[0]
    near_0 = 2.5 * centre + W1 * ones + W2 * diagonal + W4 * twos
    near_1 = W1 * centre + W2 * ones + W3 * diagonal
    near_2 = W4 * centre

    def planes(p):
        return [corner_sums(v) for v in get3(field, p)]

    put_corners(corners, planes(6))

    def step(p, n):
        news = [get_corners(corners)] + [planes(p + 1 + j) for j in range(n)]
        put_corners(corners, news[n])
        for j in range(n):
            q = p + j
            strain = strain_of(news[j + 1], news[j])
            dens = cells[q]
            worked = base[0, q] * strain[0]
            for i in range(1, 6):
                worked = worked + base[i, q] * strain[i]
            raw = explicit[q] - (0.25 * 2.97) * dens * dens * worked
            in_x = positions("gx", BX, q - 8)
            hsum = near_0 + near_1 * (in_x(-1) + in_x(1)) + near_2 * (in_x(-2) + in_x(2))
            value = jnp.where(dens > 0.0, raw / jnp.where(dens > 0.0, hsum, 1.0), 0.0)
            above, under = z_next(value), z_prev(value)
            left, right = y_next(value), y_prev(value)
            row_pair = above + under
            unit = row_pair + (left + right)
            corner = y_next(row_pair) + y_prev(row_pair)
            two = z_next(above) + z_prev(under) + y_next(left) + y_prev(right)
            near[q - 6] = (2.5 * value + W1 * unit + W2 * corner + W4 * two)[8:24]
            side[q - 6] = (W1 * value + W2 * unit + W3 * corner)[8:24]
            out[q - 6] = (W4 * value)[8:24]

    in_groups(6, 18, GROUP, step)
    for p in range(8):
        q = p + 2
        sens[p] = scale * (near[q] + (side[q - 1] + side[q + 1]) + (out[q - 2] + out[q + 2]))


def passed(block, axis, distance):
    count = lax.axis_size(axis)
    return lax.ppermute(block, axis, [(i, i + distance) for i in range(count) if 0 <= i + distance < count])


def merged(mine, other):
    larger = jnp.maximum(mine[0], other[0])
    gap = jnp.exp(jnp.minimum(mine[0], other[0]) - larger)
    first = mine[0] >= other[0]
    total = jnp.where(first, mine[1], other[1]) + jnp.where(first, other[1], mine[1]) * gap
    return jnp.stack([larger, total])


def on_device(displacement, density):
    plane = (ROWS, 128)
    up, down = kernel_call(pack_z, [(16, 8, 128)] * 2, "pack_z")(displacement, density)
    below_z, above_z = passed(up, "gz", 1), passed(down, "gz", -1)
    mid = jnp.concatenate(
        [displacement.reshape(48, 8, 128), density.reshape(16, 8, 128), below_z + above_z], axis=0
    )
    far = jnp.concatenate([mid[t : t + n] for t, n in ((0, 2), (16, 2), (32, 2), (64, 1), (68, 1), (72, 1))], axis=0)
    low, high, far = passed(mid, "gx", 1), passed(mid, "gx", -1), passed(far, "gx", -2)
    up, down = kernel_call(pack_y, [(126, 8, 128), (141, 8, 128)], "pack_y")(mid, low, high, far)
    below, above = passed(up, "gy", 1), passed(down, "gy", -1)
    (known,) = kernel_call(own_kernel, [(2, 8, 128)], "own")(mid, high, above, below)
    rounds = iter([("gy", 1), ("gy", 2), ("gy", 4), ("gx", 1), ("gx", 2), ("gx", 4), ("gz", 1), ("gz", 2)])

    def under(body, outs, name, scratch, aliases=None):
        def run(*args):
            nonlocal known
            axis, hop = next(rounds)
            other = lax.ppermute(known, axis, [(i, i ^ hop) for i in range(lax.axis_size(axis))])
            shapes = [*outs, (2, 8, 128)]
            call = kernel_call(beside(body, len(args), len(outs)), shapes, name, scratch, BUSY, aliases)
            *result, mine = call(*args, known)
            known = merged(mine, other)
            return result

        return run

    disp, line, edge, cells = under(
        widen_kernel,
        [(3, NODES, *plane), (3, NODES, 8, 128), (3, NODES, 8, 128), (CELLS, *plane)],
        "widen",
        [],
    )(mid, low, high, far, below, above)
    base, stress, highest = under(
        stress_kernel,
        [(6, CELLS, *plane), (CELLS, *plane), plane],
        "stress",
        [pltpu.VMEM((9, *plane), F32)],
    )(disp, line, edge, cells)
    rhs, stiff, weight, explicit, field, reference = under(
        load_kernel,
        [(3, CELLS, *plane), (CELLS, *plane), (CELLS, *plane), (CELLS, *plane), (3, NODES, *plane), (8, 128)],
        "load",
        [pltpu.VMEM((6, *plane), F32), pltpu.VMEM(plane, F32)],
    )(base, cells, stress, highest)
    for k in range(1, ITERS):
        (field,) = under(
            functools.partial(sweep_kernel, 1 + k, 23 - k),
            [(3, NODES, *plane)],
            f"sweep{k}",
            [pltpu.VMEM((6, *plane), F32), pltpu.VMEM((9, *plane), F32)],
            {0: 0},
        )(field, rhs, stiff, weight)
    everyone = known
    adjoint, sens, aggregate = kernel_call(
        final_kernel,
        [(3, BX, BY, BZ), (BX, BY, BZ), (8, 128)],
        "final",
        [
            pltpu.VMEM((9, *plane), F32),
            pltpu.VMEM((12, BY, 128), F32),
            pltpu.VMEM((12, BY, 128), F32),
            pltpu.VMEM((12, BY, 128), F32),
        ],
    )(field, explicit, base, cells, reference, everyone)
    return aggregate[0, 0], adjoint, sens


def solution(mesh):
    placed = (P(None, "gx", "gy", "gz"), P("gx", "gy", "gz"))
    return jax.shard_map(
        on_device,
        mesh=mesh,
        in_specs=placed,
        out_specs=(P(), P(None, "gx", "gy", "gz"), P("gx", "gy", "gz")),
        check_vma=False,
    )
```

```python
import functools
import math

import jax
import jax.numpy as jnp
from jax import lax
from jax.experimental import pallas as pl
from jax.experimental.pallas import tpu as pltpu
from jax.sharding import PartitionSpec as P

ITERS = 6
lame_first = 0.3 / (1.3 * 0.4)
shear_modulus = 1.0 / 2.6
lame_ratio = lame_first / shear_modulus
power_scale = 3.0
damping = 0.6
shift_term = 0.1
diag_factor = (lame_first + 3.0 * shear_modulus) / 16.0
W1, W2, W3 = (2.5 - math.sqrt(n) for n in (1, 2, 3))
W4 = 0.5
AXES = ("gx", "gy", "gz")

BX, BY, BZ = 8, 16, 128
NODES, CELLS = 25, 24
ROWS = 40
F32 = jnp.float32
VM = 24 * 1024 * 1024
GROUP = 3
BUSY = 20_000_000


def tile(value):
    return jax.ShapeDtypeStruct(value, F32)


def kernel_call(body, outs, name, scratch=(), flops=1_000_000, aliases=None):
    spec = pl.BlockSpec(memory_space=pltpu.VMEM)

    def run(*args):
        return pl.pallas_call(
            body,
            out_shape=[tile(shape) for shape in outs],
            in_specs=[spec] * len(args),
            out_specs=[spec] * len(outs),
            scratch_shapes=list(scratch),
            input_output_aliases=aliases or {},
            name=name,
            compiler_params=pltpu.CompilerParams(vmem_limit_bytes=VM),
            cost_estimate=pl.CostEstimate(flops=flops, bytes_accessed=1_000_000, transcendentals=0),
        )(*args)

    return run


def rolled(value, shift, axis):
    shift = shift % value.shape[axis]
    return value if shift == 0 else pltpu.roll(value, shift, axis)


def lanes():
    return lax.broadcasted_iota(jnp.int32, (8, 128), 1)


def rows():
    return lax.broadcasted_iota(jnp.int32, (8, 128), 0)


def split(value):
    return [value[8 * g : 8 * g + 8] for g in range(4)], value[32:40]


def join(main, strip):
    return jnp.concatenate([*main, strip], axis=0)


def z_next(value):
    main, strip = split(value)
    lane = lanes()
    moved = [rolled(m, -1, 1) for m in main]
    out = [jnp.where(lane == 127, rolled(strip, 127 - 32 * g, 1), moved[g]) for g in range(4)]
    tail = rolled(strip, -1, 1)
    for g in range(4):
        tail = jnp.where(lane == 32 * g + 31, rolled(main[g], 32 * g + 31, 1), tail)
    return join(out, tail)


def z_prev(value):
    main, strip = split(value)
    lane = lanes()
    moved = [rolled(m, 1, 1) for m in main]
    out = [jnp.where(lane == 0, rolled(strip, 97 - 32 * g, 1), moved[g]) for g in range(4)]
    tail = rolled(strip, 1, 1)
    for g in range(4):
        tail = jnp.where(lane == 32 * g, rolled(main[g], 32 * g + 1, 1), tail)
    return join(out, tail)


def y_next(value, beyond=None):
    main, strip = split(value)
    row = rows()
    turned = [rolled(m, -1, 0) for m in main]
    follow = [turned[1], turned[2], turned[3], turned[3] if beyond is None else beyond[0]]
    out = [jnp.where(row == 7, follow[g], turned[g]) for g in range(4)]
    tail = rolled(strip, -1, 0)
    after = rolled(tail, -32, 1)
    if beyond is not None:
        after = jnp.where(lanes() >= 96, beyond[1], after)
    return join(out, jnp.where(row == 7, after, tail))


def y_prev(value):
    main, strip = split(value)
    row = rows()
    turned = [rolled(m, 1, 0) for m in main]
    before = [turned[0], turned[0], turned[1], turned[2]]
    out = [jnp.where(row == 0, before[g], turned[g]) for g in range(4)]
    tail = rolled(strip, 1, 0)
    return join(out, jnp.where(row == 0, rolled(tail, 32, 1), tail))


def pack_z(disp, dens, up, down):
    lane = lanes()
    for c in range(4):
        for k in range(4):
            top = bottom = jnp.zeros((8, 128), F32)
            for q in range(4):
                x, t = k + 4 * (q // 2), 8 * (q % 2)
                value = disp[c, x, t : t + 8, :] if c < 3 else dens[x, t : t + 8, :]
                mine = (lane >= 32 * q) & (lane < 32 * q + 32)
                top = jnp.where(mine & (lane >= 32 * q + 24), rolled(value, 32 * q + 32, 1), top)
                bottom = jnp.where(mine & (lane < 32 * q + 9), rolled(value, 32 * q, 1), bottom)
            up[4 * c + k] = top
            down[4 * c + k] = bottom


def masked(value, real):
    return value if real is None else value * real


def pack_y(mid, low, high, far, up, down):
    lane = lanes()
    odd = (lane // 32) % 2 == 1
    sources = (low, mid, high)
    for s, src in enumerate(sources):
        real = None if s == 1 else within("gx", s - 1)
        for i in range(32):
            up[32 * s + i] = masked(src[2 * i + 1], real)
            down[32 * s + i] = masked(src[2 * i], real)
        for c in range(4):
            for k in range(2):
                first, second = src[64 + 4 * c + k], src[64 + 4 * c + k + 2]
                up[99 + 8 * s + 2 * c + k] = masked(jnp.where(odd, first, rolled(second, -32, 1)), real)
                down[99 + 8 * s + 2 * c + k] = masked(jnp.where(odd, rolled(second, 32, 1), first), real)
        for i in range(24):
            r = 24 * s + i
            down[126 + r // 8, r % 8 : r % 8 + 1, :] = masked(src[2 * i + 1, 0:1, :], real)
        for i in range(12):
            r = 12 * s + i
            down[136 + r // 8, r % 8 : r % 8 + 1, :] = masked(src[64 + i, 0:1, :], real)
    real = within("gx", 2)
    for c in range(3):
        up[96 + c] = masked(far[2 * c + 1], real)
        down[96 + c] = masked(far[2 * c], real)
        up[123 + c] = masked(far[6 + c], real)
        down[123 + c] = masked(far[6 + c], real)
        r = 72 + c
        down[126 + r // 8, r % 8 : r % 8 + 1, :] = masked(far[2 * c + 1, 0:1, :], real)
        r = 36 + c
        down[136 + r // 8, r % 8 : r % 8 + 1, :] = masked(far[6 + c, 0:1, :], real)


def unpacked(c, p, sources, far, below, above):
    lane = lanes()
    group = lane // 32
    real = (within("gx", -1), None, within("gx", 1), within("gx", 2))[p // 8]
    lower, upper = within("gy", -1), within("gy", 1)
    if p < 24:
        s, x = divmod(p, 8)
        src, i, k = sources[s], 8 * c + x, x % 4
        own = rolled(src[64 + 4 * c + k], 32 if x < 4 else -32, 1)
        slot = 99 + 8 * s + 2 * c + x % 2
        under = rolled(below[slot], {0: -32, 1: -96, 2: 0, 3: -64}[(1 if x >= 4 else 0) + (2 if k >= 2 else 0)], 1)
        over = rolled(above[slot], {0: 96, 1: 32, 2: 64, 3: 0}[(1 if x >= 4 else 0) + (2 if k >= 2 else 0)], 1)
        main = [below[32 * s + i], src[2 * i], src[2 * i + 1], above[32 * s + i]]
        r, q = 24 * s + i, 12 * s + 4 * c + k
        turn = 64 if x < 4 else 0
    else:
        own = rolled(far[6 + c], 32, 1)
        under = rolled(below[123 + c], -32, 1)
        over = rolled(above[123 + c], 96, 1)
        main = [below[96 + c], far[2 * c], far[2 * c + 1], above[96 + c]]
        r, q, turn = 72 + c, 36 + c, 64
    main = [main[0] * lower, masked(main[1], real), masked(main[2], real), main[3] * upper]
    strip = jnp.where(group == 0, under * lower, jnp.where(group == 3, over * upper, masked(own, real)))
    if c == 3:
        return join(main, strip), None
    line = jnp.broadcast_to(above[126 + r // 8, r % 8 : r % 8 + 1, :], (8, 128))
    edge = jnp.broadcast_to(above[136 + q // 8, q % 8 : q % 8 + 1, :], (8, 128))
    return join(main, strip), (line * upper, rolled(edge, turn, 1) * upper)


def corner_sums(value, beyond=None):
    if beyond is not None:
        following = y_next(value, beyond)
        both, change = following + value, following - value
        first, second = z_next(both), z_next(change)
        return first + both, second + change, first - both
    following = z_next(value)
    both, change = following + value, following - value
    after = y_next(both)
    return after + both, after - both, y_next(change) + change


def strain_of(new, old):
    grad = [[new[c][0] - old[c][0] for c in range(3)]]
    grad.append([new[c][1] + old[c][1] for c in range(3)])
    grad.append([new[c][2] + old[c][2] for c in range(3)])
    return [
        grad[0][0],
        grad[1][1],
        grad[2][2],
        grad[0][1] + grad[1][0],
        grad[1][2] + grad[2][1],
        grad[2][0] + grad[0][2],
    ]


def scaled_stress(values, factor):
    trace = lame_ratio * (values[0] + values[1] + values[2])
    return [factor * (trace + 2.0 * v) for v in values[:3]] + [factor * v for v in values[3:]]


def forces(prev, here):
    add = [prev[i] + here[i] for i in range(6)]
    sub = {i: prev[i] - here[i] for i in (0, 3, 5)}
    out = []
    for along_x, along_y, along_z in ((0, 3, 5), (3, 1, 4), (5, 4, 2)):
        a, b, w = sub[along_x], add[along_y], add[along_z]
        first = y_prev(a + b) + (a - b)
        second = y_prev(w) + w
        out.append(z_prev(first + second) + (first - second))
    return out


def get3(ref, p):
    return [ref[c, p] for c in range(3)]


def put_corners(ref, values):
    for c in range(3):
        for i in range(3):
            ref[3 * c + i] = values[c][i]


def get_corners(ref):
    return [[ref[3 * c + i] for i in range(3)] for c in range(3)]


def mises(v):
    return (
        v[0] * v[0] + v[1] * v[1] + v[2] * v[2] - v[0] * v[1] - v[1] * v[2] - v[2] * v[0]
        + 3.0 * (v[3] * v[3] + v[4] * v[4] + v[5] * v[5])
    )


def mises_slope(v):
    return [
        2.0 * v[0] - v[1] - v[2],
        2.0 * v[1] - v[2] - v[0],
        2.0 * v[2] - v[0] - v[1],
        6.0 * v[3],
        6.0 * v[4],
        6.0 * v[5],
    ]


def in_groups(lo, hi, size, body):
    full = (hi - lo) // size

    def step(i, carry):
        body(lo + size * i, size)
        return carry

    if full:
        lax.fori_loop(0, full, step, 0)
    if lo + size * full < hi:
        body(lo + size * full, hi - lo - size * full)


def own_kernel(mid, high, above, below, stats):
    lane = lanes()
    row = rows()

    def node(c, x):
        src, i, k = (mid, 8 * c + x, x % 4) if x < 8 else (high, 8 * c, 0)
        s = 1 if x < 8 else 2
        x = x % 8
        strip = src[64 + 4 * c + k]
        base = 64 if x >= 4 else 0
        far_strip = above[99 + 8 * s + 2 * c + x % 2]
        at = 64 * (x // 4) + (32 if k >= 2 else 0)
        real = None if s == 1 else within("gx", 1)
        upper = within("gy", 1)
        main = [masked(src[2 * i], real), masked(src[2 * i + 1], real), above[32 * s + i] * upper]
        strip, far_strip = masked(strip, real), far_strip * upper
        edge = [rolled(strip, 127 - base, 1), rolled(strip, 95 - base, 1), rolled(far_strip, 127 - at, 1)]
        after = [jnp.where(lane == 127, edge[t], rolled(main[t], -1, 1)) for t in range(3)]
        both = [after[t] + main[t] for t in range(3)]
        change = [after[t] - main[t] for t in range(3)]

        def follow(v):
            turned = [rolled(t, -1, 0) for t in v]
            return [jnp.where(row == 7, turned[t + 1], turned[t]) for t in range(2)]

        both_next, change_next = follow(both), follow(change)
        join2 = lambda v: jnp.concatenate(v[:2], axis=0)
        both, change, both_next, change_next = join2(both), join2(change), join2(both_next), join2(change_next)
        return both_next + both, both_next - both, change_next + change

    scores = []
    old = [node(c, 0) for c in range(3)]
    for x in range(8):
        new = [node(c, x + 1) for c in range(3)]
        values = scaled_stress(strain_of(new, old), 0.25 * shear_modulus)
        old = new
        dens = mid[48 + 2 * x : 50 + 2 * x].reshape(BY, 128)
        scores.append(power_scale * jnp.sqrt(dens * mises(values) + 1.0))
    most = functools.reduce(jnp.maximum, scores)
    top = jnp.max(most, axis=(0, 1), keepdims=True)
    total = sum(jnp.exp(score - top) for score in scores)
    total = jnp.sum(total, axis=(0, 1), keepdims=True)
    stats[0] = jnp.broadcast_to(top, (8, 128))
    stats[1] = jnp.broadcast_to(total, (8, 128))


def beside(body, ins, outs):
    def run(*refs):
        refs[ins + 1 + outs][...] = refs[ins][...]
        body(*refs[:ins], *refs[ins + 1 : ins + 1 + outs], *refs[ins + 2 + outs :])

    return run


def widen_kernel(mid, low, high, far, below, above, disp, line, edge, cells):
    sources = (low, mid, high)
    for p in range(NODES):
        for c in range(4 if p < CELLS else 3):
            value, beyond = unpacked(c, p, sources, far, below, above)
            if c == 3:
                cells[p] = value
            else:
                disp[c, p] = value
                line[c, p] = beyond[0]
                edge[c, p] = beyond[1]


def stress_kernel(disp, line, edge, cells, base, stress, highest, corners):
    def planes(p):
        return [corner_sums(disp[c, p], (line[c, p], edge[c, p])) for c in range(3)]

    put_corners(corners, planes(0))
    highest[...] = jnp.zeros((ROWS, 128), F32)

    def step(p, n):
        news = [get_corners(corners)] + [planes(p + 1 + j) for j in range(n)]
        most = highest[...]
        for j in range(n):
            values = scaled_stress(strain_of(news[j + 1], news[j]), 0.25 * shear_modulus)
            dens = cells[p + j]
            for i in range(6):
                base[i, p + j] = values[i]
            local = jnp.sqrt(dens * mises(values) + 1.0)
            stress[p + j] = local
            most = jnp.maximum(most, jnp.where(dens > 0.0, local, 0.0))
        highest[...] = most
        put_corners(corners, news[n])

    in_groups(0, CELLS, GROUP, step)


def load_kernel(base, cells, stress, highest, rhs, stiff, weight, explicit, field, reference, held, kept):
    top = power_scale * jnp.max(highest[...], axis=(0, 1), keepdims=True)
    reference[...] = jnp.broadcast_to(top, (8, 128))

    def element(p):
        dens = cells[p]
        values = [base[i, p] for i in range(6)]
        local = stress[p]
        factor = jnp.where(dens > 0.0, jnp.exp(power_scale * local - top), 0.0) / (2.0 * local)
        explicit[p] = factor * mises(values)
        part = scaled_stress(mises_slope(values), (0.25 * shear_modulus) * dens * factor)
        rigid = jnp.where(dens > 0.0, 0.01 + 0.99 * (dens * dens * dens), 0.0)
        stiff[p] = (shear_modulus / 16.0) * rigid
        return part, rigid

    part, rigid = element(0)
    for i in range(6):
        held[i] = part[i]
    kept[...] = rigid
    for c in range(3):
        field[c, 0] = jnp.zeros((ROWS, 128), F32)
        field[c, CELLS] = jnp.zeros((ROWS, 128), F32)

    def step(p, n):
        parts = [([held[i] for i in range(6)], kept[...])] + [element(p + j) for j in range(n)]
        for i in range(6):
            held[i] = parts[n][0][i]
        kept[...] = parts[n][1]
        for j in range(n):
            load = forces(parts[j][0], parts[j + 1][0])
            total = parts[j][1] + parts[j + 1][1]
            total = total + y_prev(total)
            total = total + z_prev(total)
            own = jnp.where(cells[p + j] > 0.0, damping / (diag_factor * total + shift_term), 0.0)
            weight[p + j] = own
            for c in range(3):
                value = own * load[c]
                rhs[c, p + j] = value
                field[c, p + j] = value

    in_groups(1, CELLS, GROUP, step)


def sweep_kernel(lo, hi, start, rhs, stiff, weight, field, held, corners):
    def planes(p):
        return [corner_sums(v) for v in get3(start, p)]

    def element(new, old, p):
        return scaled_stress(strain_of(new, old), stiff[p])

    first, second = planes(lo - 1), planes(lo)
    part = element(second, first, lo - 1)
    for i in range(6):
        held[i] = part[i]
    put_corners(corners, second)

    def step(p, n):
        news = [get_corners(corners)] + [planes(p + 1 + j) for j in range(n)]
        put_corners(corners, news[n])
        part = [held[i] for i in range(6)]
        for j in range(n):
            here = element(news[j + 1], news[j], p + j)
            force = forces(part, here)
            part = here
            own = weight[p + j]
            keep = 1.0 - shift_term * own
            for c in range(3):
                field[c, p + j] = keep * start[c, p + j] + rhs[c, p + j] - own * force[c]
        for i in range(6):
            held[i] = part[i]

    count = -(-(hi + 1 - lo) // GROUP) * GROUP
    in_groups(lo, lo + count, GROUP, step)


def positions(axis, length, cell):
    whole = lax.axis_size(axis) * length
    place = lax.axis_index(axis) * length + cell
    return lambda o: ((place + o >= 0) & (place + o < whole)).astype(F32)


def final_kernel(field, explicit, base, cells, reference, everyone, adjoint, sens, aggregate, corners, near, side, out):
    elements = BX * BY * BZ * lax.axis_size("gx") * lax.axis_size("gy") * lax.axis_size("gz")
    top, total = everyone[0], everyone[1]
    scale = jnp.exp(reference[...] - top) / total * float(elements)
    aggregate[...] = (top + jnp.log(total)) / power_scale
    scale = jnp.broadcast_to(scale[0:1, 0:1], (BY, 128))
    for c in range(3):
        for p in range(8):
            adjoint[c, p] = scale * field[c, 8 + p, 8:24, :]

    row = lax.broadcasted_iota(jnp.int32, (ROWS, 128), 0)
    lane = lax.broadcasted_iota(jnp.int32, (ROWS, 128), 1)
    group, place = lane // 32, lane % 32
    main = row < 32
    y_cell = jnp.where(main, row - 8, 8 * group + row - 40)
    z_cell = jnp.where(main, lane, jnp.where(place < 16, 128 + place, place - 32))
    in_y, in_z = positions("gy", BY, y_cell), positions("gz", BZ, z_cell)
    ys, zs = {o: in_y(o) for o in range(-2, 3)}, {o: in_z(o) for o in range(-2, 3)}
    beside = ys[-1] + ys[1]
    across = zs[-1] + zs[1]
    ones = beside * zs[0] + ys[0] * across
    diagonal = beside * across
    twos = (ys[-2] + ys[2]) * zs[0] + ys[0] * (zs[-2] + zs[2])
    centre = ys[0] * zs[0]
    near_0 = 2.5 * centre + W1 * ones + W2 * diagonal + W4 * twos
    near_1 = W1 * centre + W2 * ones + W3 * diagonal
    near_2 = W4 * centre

    def planes(p):
        return [corner_sums(v) for v in get3(field, p)]

    put_corners(corners, planes(6))

    def step(p, n):
        news = [get_corners(corners)] + [planes(p + 1 + j) for j in range(n)]
        put_corners(corners, news[n])
        for j in range(n):
            q = p + j
            strain = strain_of(news[j + 1], news[j])
            dens = cells[q]
            worked = base[0, q] * strain[0]
            for i in range(1, 6):
                worked = worked + base[i, q] * strain[i]
            raw = explicit[q] - (0.25 * 2.97) * dens * dens * worked
            in_x = positions("gx", BX, q - 8)
            hsum = near_0 + near_1 * (in_x(-1) + in_x(1)) + near_2 * (in_x(-2) + in_x(2))
            value = jnp.where(dens > 0.0, raw / jnp.where(dens > 0.0, hsum, 1.0), 0.0)
            above, under = z_next(value), z_prev(value)
            left, right = y_next(value), y_prev(value)
            row_pair = above + under
            unit = row_pair + (left + right)
            corner = y_next(row_pair) + y_prev(row_pair)
            two = z_next(above) + z_prev(under) + y_next(left) + y_prev(right)
            near[q - 6] = (2.5 * value + W1 * unit + W2 * corner + W4 * two)[8:24]
            side[q - 6] = (W1 * value + W2 * unit + W3 * corner)[8:24]
            out[q - 6] = (W4 * value)[8:24]

    in_groups(6, 18, GROUP, step)
    for p in range(8):
        q = p + 2
        sens[p] = scale * (near[q] + (side[q - 1] + side[q + 1]) + (out[q - 2] + out[q + 2]))


def passed(block, axis, distance):
    count = lax.axis_size(axis)
    return lax.ppermute(block, axis, [(i, (i + distance) % count) for i in range(count)])


def within(axis, distance):
    place = lax.axis_index(axis) + distance
    return ((place >= 0) & (place < lax.axis_size(axis))).astype(F32)


def merged(mine, other):
    larger = jnp.maximum(mine[0], other[0])
    gap = jnp.exp(jnp.minimum(mine[0], other[0]) - larger)
    first = mine[0] >= other[0]
    total = jnp.where(first, mine[1], other[1]) + jnp.where(first, other[1], mine[1]) * gap
    return jnp.stack([larger, total])


def on_device(displacement, density):
    plane = (ROWS, 128)
    up, down = kernel_call(pack_z, [(16, 8, 128)] * 2, "pack_z")(displacement, density)
    below_z, above_z = passed(up, "gz", 1), passed(down, "gz", -1)
    strips = below_z * within("gz", -1) + above_z * within("gz", 1)
    mid = jnp.concatenate(
        [displacement.reshape(48, 8, 128), density.reshape(16, 8, 128), strips], axis=0
    )
    far = jnp.concatenate([mid[t : t + n] for t, n in ((0, 2), (16, 2), (32, 2), (64, 1), (68, 1), (72, 1))], axis=0)
    low, high, far = passed(mid, "gx", 1), passed(mid, "gx", -1), passed(far, "gx", -2)
    up, down = kernel_call(pack_y, [(126, 8, 128), (141, 8, 128)], "pack_y")(mid, low, high, far)
    below, above = passed(up, "gy", 1), passed(down, "gy", -1)
    (known,) = kernel_call(own_kernel, [(2, 8, 128)], "own")(mid, high, above, below)
    rounds = iter([("gy", 1), ("gy", 2), ("gy", 4), ("gx", 1), ("gx", 2), ("gx", 4), ("gz", 1), ("gz", 2)])

    def under(body, outs, name, scratch, aliases=None):
        def run(*args):
            nonlocal known
            axis, hop = next(rounds)
            other = lax.ppermute(known, axis, [(i, i ^ hop) for i in range(lax.axis_size(axis))])
            shapes = [*outs, (2, 8, 128)]
            call = kernel_call(beside(body, len(args), len(outs)), shapes, name, scratch, BUSY, aliases)
            *result, mine = call(*args, known)
            known = merged(mine, other)
            return result

        return run

    disp, line, edge, cells = under(
        widen_kernel,
        [(3, NODES, *plane), (3, NODES, 8, 128), (3, NODES, 8, 128), (CELLS, *plane)],
        "widen",
        [],
    )(mid, low, high, far, below, above)
    base, stress, highest = under(
        stress_kernel,
        [(6, CELLS, *plane), (CELLS, *plane), plane],
        "stress",
        [pltpu.VMEM((9, *plane), F32)],
    )(disp, line, edge, cells)
    rhs, stiff, weight, explicit, field, reference = under(
        load_kernel,
        [(3, CELLS, *plane), (CELLS, *plane), (CELLS, *plane), (CELLS, *plane), (3, NODES, *plane), (8, 128)],
        "load",
        [pltpu.VMEM((6, *plane), F32), pltpu.VMEM(plane, F32)],
    )(base, cells, stress, highest)
    for k in range(1, ITERS):
        (field,) = under(
            functools.partial(sweep_kernel, 1 + k, 23 - k),
            [(3, NODES, *plane)],
            f"sweep{k}",
            [pltpu.VMEM((6, *plane), F32), pltpu.VMEM((9, *plane), F32)],
            {0: 0},
        )(field, rhs, stiff, weight)
    everyone = known
    adjoint, sens, aggregate = kernel_call(
        final_kernel,
        [(3, BX, BY, BZ), (BX, BY, BZ), (8, 128)],
        "final",
        [
            pltpu.VMEM((9, *plane), F32),
            pltpu.VMEM((12, BY, 128), F32),
            pltpu.VMEM((12, BY, 128), F32),
            pltpu.VMEM((12, BY, 128), F32),
        ],
    )(field, explicit, base, cells, reference, everyone)
    return aggregate[0, 0], adjoint, sens


def solution(mesh):
    placed = (P(None, "gx", "gy", "gz"), P("gx", "gy", "gz"))
    return jax.shard_map(
        on_device,
        mesh=mesh,
        in_specs=placed,
        out_specs=(P(), P(None, "gx", "gy", "gz"), P("gx", "gy", "gz")),
        check_vma=False,
    )
```

```python
import functools
import math

import jax
import jax.numpy as jnp
from jax import lax
from jax.experimental import pallas as pl
from jax.experimental.pallas import tpu as pltpu
from jax.sharding import PartitionSpec as P

ITERS = 6
lame_first = 0.3 / (1.3 * 0.4)
shear_modulus = 1.0 / 2.6
lame_ratio = lame_first / shear_modulus
power_scale = 3.0
damping = 0.6
shift_term = 0.1
diag_factor = (lame_first + 3.0 * shear_modulus) / 16.0
W1, W2, W3 = (2.5 - math.sqrt(n) for n in (1, 2, 3))
W4 = 0.5
AXES = ("gx", "gy", "gz")

BX, BY, BZ = 8, 16, 128
NODES, CELLS = 25, 24
ROWS = 40
F32 = jnp.float32
VM = 24 * 1024 * 1024
GROUP = 3
BUSY = 20_000_000


def tile(value):
    return jax.ShapeDtypeStruct(value, F32)


def kernel_call(body, outs, name, scratch=(), flops=1_000_000, aliases=None):
    spec = pl.BlockSpec(memory_space=pltpu.VMEM)

    def run(*args):
        return pl.pallas_call(
            body,
            out_shape=[tile(shape) for shape in outs],
            in_specs=[spec] * len(args),
            out_specs=[spec] * len(outs),
            scratch_shapes=list(scratch),
            input_output_aliases=aliases or {},
            name=name,
            compiler_params=pltpu.CompilerParams(vmem_limit_bytes=VM),
            cost_estimate=pl.CostEstimate(flops=flops, bytes_accessed=1_000_000, transcendentals=0),
        )(*args)

    return run


def rolled(value, shift, axis):
    shift = shift % value.shape[axis]
    return value if shift == 0 else pltpu.roll(value, shift, axis)


def lanes():
    return lax.broadcasted_iota(jnp.int32, (8, 128), 1)


def rows():
    return lax.broadcasted_iota(jnp.int32, (8, 128), 0)


def split(value):
    return [value[8 * g : 8 * g + 8] for g in range(4)], value[32:40]


def join(main, strip):
    return jnp.concatenate([*main, strip], axis=0)


def z_next(value):
    main, strip = split(value)
    last = lanes() == 127
    out = [jnp.where(last, rolled(strip, 120 - 32 * g, 1), rolled(main[g], -1, 1)) for g in range(4)]
    return join(out, rolled(strip, -1, 1))


def z_prev(value):
    main, strip = split(value)
    first = lanes() == 0
    out = [jnp.where(first, rolled(strip, -23 - 32 * g, 1), rolled(main[g], 1, 1)) for g in range(4)]
    return join(out, rolled(strip, 1, 1))


def y_next(value, beyond=None):
    main, strip = split(value)
    row = rows()
    turned = [rolled(m, -1, 0) for m in main]
    follow = [turned[1], turned[2], turned[3], turned[3] if beyond is None else beyond[0]]
    out = [jnp.where(row == 7, follow[g], turned[g]) for g in range(4)]
    tail = rolled(strip, -1, 0)
    after = rolled(tail, -32, 1)
    if beyond is not None:
        after = jnp.where(lanes() >= 96, beyond[1], after)
    return join(out, jnp.where(row == 7, after, tail))


def y_prev(value):
    main, strip = split(value)
    row = rows()
    turned = [rolled(m, 1, 0) for m in main]
    before = [turned[0], turned[0], turned[1], turned[2]]
    out = [jnp.where(row == 0, before[g], turned[g]) for g in range(4)]
    tail = rolled(strip, 1, 0)
    return join(out, jnp.where(row == 0, rolled(tail, 32, 1), tail))


def pack_z(disp, dens, up, down, inner):
    lane = lanes()
    for c in range(4):
        short = 0 if c < 3 else 1
        for k in range(4):
            top = bottom = own = jnp.zeros((8, 128), F32)
            for q in range(4):
                x, t = k + 4 * (q // 2), 8 * (q % 2)
                value = disp[c, x, t : t + 8, :] if c < 3 else dens[x, t : t + 8, :]
                place = lane - 32 * q
                top = jnp.where((place >= 16) & (place < 24), rolled(value, 32 * q + 24, 1), top)
                bottom = jnp.where((place >= 7) & (place < 16 - short), rolled(value, 32 * q + 7, 1), bottom)
                own = jnp.where((place >= 24) & (place < 32 - short), rolled(value, 32 * q + 24, 1), own)
                own = jnp.where((place >= 0) & (place < 7), rolled(value, 32 * q + 7, 1), own)
            up[4 * c + k] = top
            down[4 * c + k] = bottom
            inner[4 * c + k] = own


def masked(value, real):
    return value if real is None else value * real


def pack_y(mid, low, high, far, up, down):
    lane = lanes()
    odd = (lane // 32) % 2 == 1
    sources = (low, mid, high)
    for s, src in enumerate(sources):
        real = None if s == 1 else within("gx", s - 1)
        for i in range(32):
            up[32 * s + i] = masked(src[2 * i + 1], real)
            down[32 * s + i] = masked(src[2 * i], real)
        for c in range(4):
            for k in range(2):
                first, second = src[64 + 4 * c + k], src[64 + 4 * c + k + 2]
                up[99 + 8 * s + 2 * c + k] = masked(jnp.where(odd, first, rolled(second, -32, 1)), real)
                down[99 + 8 * s + 2 * c + k] = masked(jnp.where(odd, rolled(second, 32, 1), first), real)
        for i in range(24):
            r = 24 * s + i
            down[126 + r // 8, r % 8 : r % 8 + 1, :] = masked(src[2 * i + 1, 0:1, :], real)
        for i in range(12):
            r = 12 * s + i
            down[136 + r // 8, r % 8 : r % 8 + 1, :] = masked(src[64 + i, 0:1, :], real)
    real = within("gx", 2)
    for c in range(3):
        up[96 + c] = masked(far[2 * c + 1], real)
        down[96 + c] = masked(far[2 * c], real)
        up[123 + c] = masked(far[6 + c], real)
        down[123 + c] = masked(far[6 + c], real)
        r = 72 + c
        down[126 + r // 8, r % 8 : r % 8 + 1, :] = masked(far[2 * c + 1, 0:1, :], real)
        r = 36 + c
        down[136 + r // 8, r % 8 : r % 8 + 1, :] = masked(far[6 + c, 0:1, :], real)


def unpacked(c, p, sources, far, below, above):
    lane = lanes()
    group = lane // 32
    real = (within("gx", -1), None, within("gx", 1), within("gx", 2))[p // 8]
    lower, upper = within("gy", -1), within("gy", 1)
    if p < 24:
        s, x = divmod(p, 8)
        src, i, k = sources[s], 8 * c + x, x % 4
        own = rolled(src[64 + 4 * c + k], 32 if x < 4 else -32, 1)
        slot = 99 + 8 * s + 2 * c + x % 2
        under = rolled(below[slot], {0: -32, 1: -96, 2: 0, 3: -64}[(1 if x >= 4 else 0) + (2 if k >= 2 else 0)], 1)
        over = rolled(above[slot], {0: 96, 1: 32, 2: 64, 3: 0}[(1 if x >= 4 else 0) + (2 if k >= 2 else 0)], 1)
        main = [below[32 * s + i], src[2 * i], src[2 * i + 1], above[32 * s + i]]
        r, q = 24 * s + i, 12 * s + 4 * c + k
        turn = 64 if x < 4 else 0
    else:
        own = rolled(far[6 + c], 32, 1)
        under = rolled(below[123 + c], -32, 1)
        over = rolled(above[123 + c], 96, 1)
        main = [below[96 + c], far[2 * c], far[2 * c + 1], above[96 + c]]
        r, q, turn = 72 + c, 36 + c, 64
    main = [main[0] * lower, masked(main[1], real), masked(main[2], real), main[3] * upper]
    strip = jnp.where(group == 0, under * lower, jnp.where(group == 3, over * upper, masked(own, real)))
    if c == 3:
        return join(main, strip), None
    line = jnp.broadcast_to(above[126 + r // 8, r % 8 : r % 8 + 1, :], (8, 128))
    edge = jnp.broadcast_to(above[136 + q // 8, q % 8 : q % 8 + 1, :], (8, 128))
    return join(main, strip), (line * upper, rolled(edge, turn, 1) * upper)


def corner_sums(value, beyond=None):
    if beyond is not None:
        following = y_next(value, beyond)
        both, change = following + value, following - value
        first, second = z_next(both), z_next(change)
        return first + both, second + change, first - both
    following = z_next(value)
    both, change = following + value, following - value
    after = y_next(both)
    return after + both, after - both, y_next(change) + change


def strain_of(new, old):
    grad = [[new[c][0] - old[c][0] for c in range(3)]]
    grad.append([new[c][1] + old[c][1] for c in range(3)])
    grad.append([new[c][2] + old[c][2] for c in range(3)])
    return [
        grad[0][0],
        grad[1][1],
        grad[2][2],
        grad[0][1] + grad[1][0],
        grad[1][2] + grad[2][1],
        grad[2][0] + grad[0][2],
    ]


def scaled_stress(values, factor):
    trace = lame_ratio * (values[0] + values[1] + values[2])
    return [factor * (trace + 2.0 * v) for v in values[:3]] + [factor * v for v in values[3:]]


def forces(prev, here):
    add = [prev[i] + here[i] for i in range(6)]
    sub = {i: prev[i] - here[i] for i in (0, 3, 5)}
    out = []
    for along_x, along_y, along_z in ((0, 3, 5), (3, 1, 4), (5, 4, 2)):
        a, b, w = sub[along_x], add[along_y], add[along_z]
        first = y_prev(a + b) + (a - b)
        second = y_prev(w) + w
        out.append(z_prev(first + second) + (first - second))
    return out


def get3(ref, p):
    return [ref[c, p] for c in range(3)]


def put_corners(ref, values):
    for c in range(3):
        for i in range(3):
            ref[3 * c + i] = values[c][i]


def get_corners(ref):
    return [[ref[3 * c + i] for i in range(3)] for c in range(3)]


def mises(v):
    return (
        v[0] * v[0] + v[1] * v[1] + v[2] * v[2] - v[0] * v[1] - v[1] * v[2] - v[2] * v[0]
        + 3.0 * (v[3] * v[3] + v[4] * v[4] + v[5] * v[5])
    )


def mises_slope(v):
    return [
        2.0 * v[0] - v[1] - v[2],
        2.0 * v[1] - v[2] - v[0],
        2.0 * v[2] - v[0] - v[1],
        6.0 * v[3],
        6.0 * v[4],
        6.0 * v[5],
    ]


def in_groups(lo, hi, size, body):
    full = (hi - lo) // size

    def step(i, carry):
        body(lo + size * i, size)
        return carry

    if full:
        lax.fori_loop(0, full, step, 0)
    if lo + size * full < hi:
        body(lo + size * full, hi - lo - size * full)


def own_kernel(mid, high, above, below, stats):
    lane = lanes()
    row = rows()

    def node(c, x):
        src, i, k = (mid, 8 * c + x, x % 4) if x < 8 else (high, 8 * c, 0)
        s = 1 if x < 8 else 2
        x = x % 8
        strip = src[64 + 4 * c + k]
        base = 64 if x >= 4 else 0
        far_strip = above[99 + 8 * s + 2 * c + x % 2]
        at = 64 * (x // 4) + (32 if k >= 2 else 0)
        real = None if s == 1 else within("gx", 1)
        upper = within("gy", 1)
        main = [masked(src[2 * i], real), masked(src[2 * i + 1], real), above[32 * s + i] * upper]
        strip, far_strip = masked(strip, real), far_strip * upper
        edge = [rolled(strip, 120 - base, 1), rolled(strip, 88 - base, 1), rolled(far_strip, 120 - at, 1)]
        after = [jnp.where(lane == 127, edge[t], rolled(main[t], -1, 1)) for t in range(3)]
        both = [after[t] + main[t] for t in range(3)]
        change = [after[t] - main[t] for t in range(3)]

        def follow(v):
            turned = [rolled(t, -1, 0) for t in v]
            return [jnp.where(row == 7, turned[t + 1], turned[t]) for t in range(2)]

        both_next, change_next = follow(both), follow(change)
        join2 = lambda v: jnp.concatenate(v[:2], axis=0)
        both, change, both_next, change_next = join2(both), join2(change), join2(both_next), join2(change_next)
        return both_next + both, both_next - both, change_next + change

    scores = []
    old = [node(c, 0) for c in range(3)]
    for x in range(8):
        new = [node(c, x + 1) for c in range(3)]
        values = scaled_stress(strain_of(new, old), 0.25 * shear_modulus)
        old = new
        dens = mid[48 + 2 * x : 50 + 2 * x].reshape(BY, 128)
        scores.append(power_scale * jnp.sqrt(dens * mises(values) + 1.0))
    most = functools.reduce(jnp.maximum, scores)
    top = jnp.max(most, axis=(0, 1), keepdims=True)
    total = sum(jnp.exp(score - top) for score in scores)
    total = jnp.sum(total, axis=(0, 1), keepdims=True)
    stats[0] = jnp.broadcast_to(top, (8, 128))
    stats[1] = jnp.broadcast_to(total, (8, 128))


def beside(body, ins, outs):
    def run(*refs):
        refs[ins + 1 + outs][...] = refs[ins][...]
        body(*refs[:ins], *refs[ins + 1 : ins + 1 + outs], *refs[ins + 2 + outs :])

    return run


def widen_kernel(mid, low, high, far, below, above, disp, line, edge, cells):
    sources = (low, mid, high)
    for p in range(NODES):
        for c in range(4 if p < CELLS else 3):
            value, beyond = unpacked(c, p, sources, far, below, above)
            if c == 3:
                cells[p] = value
            else:
                disp[c, p] = value
                line[c, p] = beyond[0]
                edge[c, p] = beyond[1]


def stress_kernel(disp, line, edge, cells, base, stress, highest, corners):
    def planes(p):
        return [corner_sums(disp[c, p], (line[c, p], edge[c, p])) for c in range(3)]

    put_corners(corners, planes(0))
    highest[...] = jnp.zeros((ROWS, 128), F32)

    def step(p, n):
        news = [get_corners(corners)] + [planes(p + 1 + j) for j in range(n)]
        most = highest[...]
        for j in range(n):
            values = scaled_stress(strain_of(news[j + 1], news[j]), 0.25 * shear_modulus)
            dens = cells[p + j]
            for i in range(6):
                base[i, p + j] = values[i]
            local = jnp.sqrt(dens * mises(values) + 1.0)
            stress[p + j] = local
            most = jnp.maximum(most, jnp.where(dens > 0.0, local, 0.0))
        highest[...] = most
        put_corners(corners, news[n])

    in_groups(0, CELLS, GROUP, step)


def load_kernel(base, cells, stress, highest, rhs, stiff, weight, explicit, field, reference, held, kept):
    top = power_scale * jnp.max(highest[...], axis=(0, 1), keepdims=True)
    reference[...] = jnp.broadcast_to(top, (8, 128))

    def element(p):
        dens = cells[p]
        values = [base[i, p] for i in range(6)]
        local = stress[p]
        factor = jnp.where(dens > 0.0, jnp.exp(power_scale * local - top), 0.0) / (2.0 * local)
        explicit[p] = factor * mises(values)
        part = scaled_stress(mises_slope(values), (0.25 * shear_modulus) * dens * factor)
        rigid = jnp.where(dens > 0.0, 0.01 + 0.99 * (dens * dens * dens), 0.0)
        stiff[p] = (shear_modulus / 16.0) * rigid
        return part, rigid

    part, rigid = element(0)
    for i in range(6):
        held[i] = part[i]
    kept[...] = rigid
    for c in range(3):
        field[c, 0] = jnp.zeros((ROWS, 128), F32)
        field[c, CELLS] = jnp.zeros((ROWS, 128), F32)

    def step(p, n):
        parts = [([held[i] for i in range(6)], kept[...])] + [element(p + j) for j in range(n)]
        for i in range(6):
            held[i] = parts[n][0][i]
        kept[...] = parts[n][1]
        for j in range(n):
            load = forces(parts[j][0], parts[j + 1][0])
            total = parts[j][1] + parts[j + 1][1]
            total = total + y_prev(total)
            total = total + z_prev(total)
            own = jnp.where(cells[p + j] > 0.0, damping / (diag_factor * total + shift_term), 0.0)
            weight[p + j] = own
            for c in range(3):
                value = own * load[c]
                rhs[c, p + j] = value
                field[c, p + j] = value

    in_groups(1, CELLS, GROUP, step)


def sweep_kernel(lo, hi, start, rhs, stiff, weight, field, held, corners):
    def planes(p):
        return [corner_sums(v) for v in get3(start, p)]

    def element(new, old, p):
        return scaled_stress(strain_of(new, old), stiff[p])

    first, second = planes(lo - 1), planes(lo)
    part = element(second, first, lo - 1)
    for i in range(6):
        held[i] = part[i]
    put_corners(corners, second)

    def step(p, n):
        news = [get_corners(corners)] + [planes(p + 1 + j) for j in range(n)]
        put_corners(corners, news[n])
        part = [held[i] for i in range(6)]
        for j in range(n):
            here = element(news[j + 1], news[j], p + j)
            force = forces(part, here)
            part = here
            own = weight[p + j]
            keep = 1.0 - shift_term * own
            for c in range(3):
                field[c, p + j] = keep * start[c, p + j] + rhs[c, p + j] - own * force[c]
        for i in range(6):
            held[i] = part[i]

    count = -(-(hi + 1 - lo) // GROUP) * GROUP
    in_groups(lo, lo + count, GROUP, step)


def positions(axis, length, cell):
    whole = lax.axis_size(axis) * length
    place = lax.axis_index(axis) * length + cell
    return lambda o: ((place + o >= 0) & (place + o < whole)).astype(F32)


def final_kernel(field, explicit, base, cells, reference, everyone, adjoint, sens, aggregate, corners, near, side, out):
    elements = BX * BY * BZ * lax.axis_size("gx") * lax.axis_size("gy") * lax.axis_size("gz")
    top, total = everyone[0], everyone[1]
    scale = jnp.exp(reference[...] - top) / total * float(elements)
    aggregate[...] = (top + jnp.log(total)) / power_scale
    scale = jnp.broadcast_to(scale[0:1, 0:1], (BY, 128))
    for c in range(3):
        for p in range(8):
            adjoint[c, p] = scale * field[c, 8 + p, 8:24, :]

    row = lax.broadcasted_iota(jnp.int32, (ROWS, 128), 0)
    lane = lax.broadcasted_iota(jnp.int32, (ROWS, 128), 1)
    group, place = lane // 32, lane % 32
    main = row < 32
    y_cell = jnp.where(main, row - 8, 8 * group + row - 40)
    z_cell = jnp.where(main, lane, jnp.where(place < 16, 121 + place, place - 24))
    in_y, in_z = positions("gy", BY, y_cell), positions("gz", BZ, z_cell)
    ys, zs = {o: in_y(o) for o in range(-2, 3)}, {o: in_z(o) for o in range(-2, 3)}
    beside = ys[-1] + ys[1]
    across = zs[-1] + zs[1]
    ones = beside * zs[0] + ys[0] * across
    diagonal = beside * across
    twos = (ys[-2] + ys[2]) * zs[0] + ys[0] * (zs[-2] + zs[2])
    centre = ys[0] * zs[0]
    near_0 = 2.5 * centre + W1 * ones + W2 * diagonal + W4 * twos
    near_1 = W1 * centre + W2 * ones + W3 * diagonal
    near_2 = W4 * centre

    def planes(p):
        return [corner_sums(v) for v in get3(field, p)]

    put_corners(corners, planes(6))

    def step(p, n):
        news = [get_corners(corners)] + [planes(p + 1 + j) for j in range(n)]
        put_corners(corners, news[n])
        for j in range(n):
            q = p + j
            strain = strain_of(news[j + 1], news[j])
            dens = cells[q]
            worked = base[0, q] * strain[0]
            for i in range(1, 6):
                worked = worked + base[i, q] * strain[i]
            raw = explicit[q] - (0.25 * 2.97) * dens * dens * worked
            in_x = positions("gx", BX, q - 8)
            hsum = near_0 + near_1 * (in_x(-1) + in_x(1)) + near_2 * (in_x(-2) + in_x(2))
            value = jnp.where(dens > 0.0, raw / jnp.where(dens > 0.0, hsum, 1.0), 0.0)
            above, under = z_next(value), z_prev(value)
            left, right = y_next(value), y_prev(value)
            row_pair = above + under
            unit = row_pair + (left + right)
            corner = y_next(row_pair) + y_prev(row_pair)
            two = z_next(above) + z_prev(under) + y_next(left) + y_prev(right)
            near[q - 6] = (2.5 * value + W1 * unit + W2 * corner + W4 * two)[8:24]
            side[q - 6] = (W1 * value + W2 * unit + W3 * corner)[8:24]
            out[q - 6] = (W4 * value)[8:24]

    in_groups(6, 18, GROUP, step)
    for p in range(8):
        q = p + 2
        sens[p] = scale * (near[q] + (side[q - 1] + side[q + 1]) + (out[q - 2] + out[q + 2]))


def passed(block, axis, distance):
    count = lax.axis_size(axis)
    return lax.ppermute(block, axis, [(i, (i + distance) % count) for i in range(count)])


def within(axis, distance):
    place = lax.axis_index(axis) + distance
    return ((place >= 0) & (place < lax.axis_size(axis))).astype(F32)


def merged(mine, other):
    larger = jnp.maximum(mine[0], other[0])
    gap = jnp.exp(jnp.minimum(mine[0], other[0]) - larger)
    first = mine[0] >= other[0]
    total = jnp.where(first, mine[1], other[1]) + jnp.where(first, other[1], mine[1]) * gap
    return jnp.stack([larger, total])


def on_device(displacement, density):
    plane = (ROWS, 128)
    up, down, inner = kernel_call(pack_z, [(16, 8, 128)] * 3, "pack_z")(displacement, density)
    below_z, above_z = passed(up, "gz", 1), passed(down, "gz", -1)
    strips = inner + below_z * within("gz", -1) + above_z * within("gz", 1)
    mid = jnp.concatenate(
        [displacement.reshape(48, 8, 128), density.reshape(16, 8, 128), strips], axis=0
    )
    far = jnp.concatenate([mid[t : t + n] for t, n in ((0, 2), (16, 2), (32, 2), (64, 1), (68, 1), (72, 1))], axis=0)
    low, high, far = passed(mid, "gx", 1), passed(mid, "gx", -1), passed(far, "gx", -2)
    up, down = kernel_call(pack_y, [(126, 8, 128), (141, 8, 128)], "pack_y")(mid, low, high, far)
    below, above = passed(up, "gy", 1), passed(down, "gy", -1)
    (known,) = kernel_call(own_kernel, [(2, 8, 128)], "own")(mid, high, above, below)
    rounds = iter([("gy", 1), ("gy", 2), ("gy", 4), ("gx", 1), ("gx", 2), ("gx", 4), ("gz", 1), ("gz", 2)])

    def under(body, outs, name, scratch, aliases=None):
        def run(*args):
            nonlocal known
            axis, hop = next(rounds)
            other = lax.ppermute(known, axis, [(i, i ^ hop) for i in range(lax.axis_size(axis))])
            shapes = [*outs, (2, 8, 128)]
            call = kernel_call(beside(body, len(args), len(outs)), shapes, name, scratch, BUSY, aliases)
            *result, mine = call(*args, known)
            known = merged(mine, other)
            return result

        return run

    disp, line, edge, cells = under(
        widen_kernel,
        [(3, NODES, *plane), (3, NODES, 8, 128), (3, NODES, 8, 128), (CELLS, *plane)],
        "widen",
        [],
    )(mid, low, high, far, below, above)
    base, stress, highest = under(
        stress_kernel,
        [(6, CELLS, *plane), (CELLS, *plane), plane],
        "stress",
        [pltpu.VMEM((9, *plane), F32)],
    )(disp, line, edge, cells)
    rhs, stiff, weight, explicit, field, reference = under(
        load_kernel,
        [(3, CELLS, *plane), (CELLS, *plane), (CELLS, *plane), (CELLS, *plane), (3, NODES, *plane), (8, 128)],
        "load",
        [pltpu.VMEM((6, *plane), F32), pltpu.VMEM(plane, F32)],
    )(base, cells, stress, highest)
    for k in range(1, ITERS):
        (field,) = under(
            functools.partial(sweep_kernel, 1 + k, 23 - k),
            [(3, NODES, *plane)],
            f"sweep{k}",
            [pltpu.VMEM((6, *plane), F32), pltpu.VMEM((9, *plane), F32)],
            {0: 0},
        )(field, rhs, stiff, weight)
    everyone = known
    adjoint, sens, aggregate = kernel_call(
        final_kernel,
        [(3, BX, BY, BZ), (BX, BY, BZ), (8, 128)],
        "final",
        [
            pltpu.VMEM((9, *plane), F32),
            pltpu.VMEM((12, BY, 128), F32),
            pltpu.VMEM((12, BY, 128), F32),
            pltpu.VMEM((12, BY, 128), F32),
        ],
    )(field, explicit, base, cells, reference, everyone)
    return aggregate[0, 0], adjoint, sens


def solution(mesh):
    placed = (P(None, "gx", "gy", "gz"), P("gx", "gy", "gz"))
    return jax.shard_map(
        on_device,
        mesh=mesh,
        in_specs=placed,
        out_specs=(P(), P(None, "gx", "gy", "gz"), P("gx", "gy", "gz")),
        check_vma=False,
    )
```

```python
import functools
import math

import jax
import jax.numpy as jnp
from jax import lax
from jax.experimental import pallas as pl
from jax.experimental.pallas import tpu as pltpu
from jax.sharding import PartitionSpec as P

ITERS = 6
lame_first = 0.3 / (1.3 * 0.4)
shear_modulus = 1.0 / 2.6
lame_ratio = lame_first / shear_modulus
power_scale = 3.0
damping = 0.6
shift_term = 0.1
diag_factor = (lame_first + 3.0 * shear_modulus) / 16.0
W1, W2, W3 = (2.5 - math.sqrt(n) for n in (1, 2, 3))
W4 = 0.5
AXES = ("gx", "gy", "gz")

BX, BY, BZ = 8, 16, 128
NODES, CELLS = 25, 24
ROWS = 40
F32 = jnp.float32
VM = 24 * 1024 * 1024
GROUP = 3
BUSY = 20_000_000


def tile(value):
    return jax.ShapeDtypeStruct(value, F32)


def kernel_call(body, outs, name, scratch=(), flops=1_000_000, aliases=None):
    spec = pl.BlockSpec(memory_space=pltpu.VMEM)

    def run(*args):
        return pl.pallas_call(
            body,
            out_shape=[tile(shape) for shape in outs],
            in_specs=[spec] * len(args),
            out_specs=[spec] * len(outs),
            scratch_shapes=list(scratch),
            input_output_aliases=aliases or {},
            name=name,
            compiler_params=pltpu.CompilerParams(vmem_limit_bytes=VM),
            cost_estimate=pl.CostEstimate(flops=flops, bytes_accessed=1_000_000, transcendentals=0),
        )(*args)

    return run


def rolled(value, shift, axis):
    shift = shift % value.shape[axis]
    return value if shift == 0 else pltpu.roll(value, shift, axis)


def lanes():
    return lax.broadcasted_iota(jnp.int32, (8, 128), 1)


def rows():
    return lax.broadcasted_iota(jnp.int32, (8, 128), 0)


def split(value):
    return [value[8 * g : 8 * g + 8] for g in range(4)], value[32:40]


def join(main, strip):
    return jnp.concatenate([*main, strip], axis=0)


def z_next(value):
    main, strip = split(value)
    last = lanes() == 127
    out = [jnp.where(last, rolled(strip, 120 - 32 * g, 1), rolled(main[g], -1, 1)) for g in range(4)]
    return join(out, rolled(strip, -1, 1))


def z_prev(value):
    main, strip = split(value)
    first = lanes() == 0
    out = [jnp.where(first, rolled(strip, -23 - 32 * g, 1), rolled(main[g], 1, 1)) for g in range(4)]
    return join(out, rolled(strip, 1, 1))


def y_next(value, beyond=None):
    main, strip = split(value)
    row = rows()
    turned = [rolled(m, -1, 0) for m in main]
    follow = [turned[1], turned[2], turned[3], turned[3] if beyond is None else beyond[0]]
    out = [jnp.where(row == 7, follow[g], turned[g]) for g in range(4)]
    tail = rolled(strip, -1, 0)
    after = rolled(tail, -32, 1)
    if beyond is not None:
        after = jnp.where(lanes() >= 96, beyond[1], after)
    return join(out, jnp.where(row == 7, after, tail))


def y_prev(value):
    main, strip = split(value)
    row = rows()
    turned = [rolled(m, 1, 0) for m in main]
    before = [turned[0], turned[0], turned[1], turned[2]]
    out = [jnp.where(row == 0, before[g], turned[g]) for g in range(4)]
    tail = rolled(strip, 1, 0)
    return join(out, jnp.where(row == 0, rolled(tail, 32, 1), tail))


def pack_z(main, up, down, inner, first):
    lane = lanes()
    for c in range(4):
        short = 0 if c < 3 else 1
        for k in range(4):
            top = bottom = own = jnp.zeros((8, 128), F32)
            for q in range(4):
                value = main[16 * c + 2 * (k + 4 * (q // 2)) + q % 2]
                place = lane - 32 * q
                top = jnp.where((place >= 16) & (place < 24), rolled(value, 32 * q + 24, 1), top)
                bottom = jnp.where((place >= 7) & (place < 16 - short), rolled(value, 32 * q + 7, 1), bottom)
                own = jnp.where((place >= 24) & (place < 32 - short), rolled(value, 32 * q + 24, 1), own)
                own = jnp.where((place >= 0) & (place < 7), rolled(value, 32 * q + 7, 1), own)
            if k == 0 and c < 3:
                first[2 * c] = main[16 * c]
                first[2 * c + 1] = main[16 * c + 1]
            up[4 * c + k] = top
            down[4 * c + k] = bottom
            inner[4 * c + k] = own


def masked(value, real):
    return value if real is None else value * real


def pack_y(mid, low, high, far, up, down):
    lane = lanes()
    odd = (lane // 32) % 2 == 1
    sources = (low, mid, high)
    for s, src in enumerate(sources):
        real = None if s == 1 else within("gx", s - 1)
        for i in range(32):
            up[32 * s + i] = masked(src[2 * i + 1], real)
            down[32 * s + i] = masked(src[2 * i], real)
        for c in range(4):
            for k in range(2):
                first, second = src[64 + 4 * c + k], src[64 + 4 * c + k + 2]
                up[99 + 8 * s + 2 * c + k] = masked(jnp.where(odd, first, rolled(second, -32, 1)), real)
                down[99 + 8 * s + 2 * c + k] = masked(jnp.where(odd, rolled(second, 32, 1), first), real)
        for i in range(24):
            r = 24 * s + i
            down[126 + r // 8, r % 8 : r % 8 + 1, :] = masked(src[2 * i + 1, 0:1, :], real)
        for i in range(12):
            r = 12 * s + i
            down[136 + r // 8, r % 8 : r % 8 + 1, :] = masked(src[64 + i, 0:1, :], real)
    real = within("gx", 2)
    for c in range(3):
        up[96 + c] = masked(far[2 * c + 1], real)
        down[96 + c] = masked(far[2 * c], real)
        up[123 + c] = masked(far[6 + c], real)
        down[123 + c] = masked(far[6 + c], real)
        r = 72 + c
        down[126 + r // 8, r % 8 : r % 8 + 1, :] = masked(far[2 * c + 1, 0:1, :], real)
        r = 36 + c
        down[136 + r // 8, r % 8 : r % 8 + 1, :] = masked(far[6 + c, 0:1, :], real)


def unpacked(c, p, sources, far, below, above):
    lane = lanes()
    group = lane // 32
    real = (within("gx", -1), None, within("gx", 1), within("gx", 2))[p // 8]
    lower, upper = within("gy", -1), within("gy", 1)
    if p < 24:
        s, x = divmod(p, 8)
        src, i, k = sources[s], 8 * c + x, x % 4
        own = rolled(src[64 + 4 * c + k], 32 if x < 4 else -32, 1)
        slot = 99 + 8 * s + 2 * c + x % 2
        under = rolled(below[slot], {0: -32, 1: -96, 2: 0, 3: -64}[(1 if x >= 4 else 0) + (2 if k >= 2 else 0)], 1)
        over = rolled(above[slot], {0: 96, 1: 32, 2: 64, 3: 0}[(1 if x >= 4 else 0) + (2 if k >= 2 else 0)], 1)
        main = [below[32 * s + i], src[2 * i], src[2 * i + 1], above[32 * s + i]]
        r, q = 24 * s + i, 12 * s + 4 * c + k
        turn = 64 if x < 4 else 0
    else:
        own = rolled(far[6 + c], 32, 1)
        under = rolled(below[123 + c], -32, 1)
        over = rolled(above[123 + c], 96, 1)
        main = [below[96 + c], far[2 * c], far[2 * c + 1], above[96 + c]]
        r, q, turn = 72 + c, 36 + c, 64
    main = [main[0] * lower, masked(main[1], real), masked(main[2], real), main[3] * upper]
    strip = jnp.where(group == 0, under * lower, jnp.where(group == 3, over * upper, masked(own, real)))
    if c == 3:
        return join(main, strip), None
    line = jnp.broadcast_to(above[126 + r // 8, r % 8 : r % 8 + 1, :], (8, 128))
    edge = jnp.broadcast_to(above[136 + q // 8, q % 8 : q % 8 + 1, :], (8, 128))
    return join(main, strip), (line * upper, rolled(edge, turn, 1) * upper)


def corner_sums(value, beyond=None):
    if beyond is not None:
        following = y_next(value, beyond)
        both, change = following + value, following - value
        first, second = z_next(both), z_next(change)
        return first + both, second + change, first - both
    following = z_next(value)
    both, change = following + value, following - value
    after = y_next(both)
    return after + both, after - both, y_next(change) + change


def strain_of(new, old):
    grad = [[new[c][0] - old[c][0] for c in range(3)]]
    grad.append([new[c][1] + old[c][1] for c in range(3)])
    grad.append([new[c][2] + old[c][2] for c in range(3)])
    return [
        grad[0][0],
        grad[1][1],
        grad[2][2],
        grad[0][1] + grad[1][0],
        grad[1][2] + grad[2][1],
        grad[2][0] + grad[0][2],
    ]


def scaled_stress(values, factor):
    trace = lame_ratio * (values[0] + values[1] + values[2])
    return [factor * (trace + 2.0 * v) for v in values[:3]] + [factor * v for v in values[3:]]


def forces(prev, here):
    add = [prev[i] + here[i] for i in range(6)]
    sub = {i: prev[i] - here[i] for i in (0, 3, 5)}
    out = []
    for along_x, along_y, along_z in ((0, 3, 5), (3, 1, 4), (5, 4, 2)):
        a, b, w = sub[along_x], add[along_y], add[along_z]
        first = y_prev(a + b) + (a - b)
        second = y_prev(w) + w
        out.append(z_prev(first + second) + (first - second))
    return out


def get3(ref, p):
    return [ref[c, p] for c in range(3)]


def put_corners(ref, values):
    for c in range(3):
        for i in range(3):
            ref[3 * c + i] = values[c][i]


def get_corners(ref):
    return [[ref[3 * c + i] for i in range(3)] for c in range(3)]


def mises(v):
    return (
        v[0] * v[0] + v[1] * v[1] + v[2] * v[2] - v[0] * v[1] - v[1] * v[2] - v[2] * v[0]
        + 3.0 * (v[3] * v[3] + v[4] * v[4] + v[5] * v[5])
    )


def mises_slope(v):
    return [
        2.0 * v[0] - v[1] - v[2],
        2.0 * v[1] - v[2] - v[0],
        2.0 * v[2] - v[0] - v[1],
        6.0 * v[3],
        6.0 * v[4],
        6.0 * v[5],
    ]


def in_groups(lo, hi, size, body):
    full = (hi - lo) // size

    def step(i, carry):
        body(lo + size * i, size)
        return carry

    if full:
        lax.fori_loop(0, full, step, 0)
    if lo + size * full < hi:
        body(lo + size * full, hi - lo - size * full)


def own_kernel(mid, high, above, below, stats):
    lane = lanes()
    row = rows()

    def node(c, x):
        src, i, k = (mid, 8 * c + x, x % 4) if x < 8 else (high, 8 * c, 0)
        s = 1 if x < 8 else 2
        x = x % 8
        strip = src[64 + 4 * c + k]
        base = 64 if x >= 4 else 0
        far_strip = above[99 + 8 * s + 2 * c + x % 2]
        at = 64 * (x // 4) + (32 if k >= 2 else 0)
        real = None if s == 1 else within("gx", 1)
        upper = within("gy", 1)
        main = [masked(src[2 * i], real), masked(src[2 * i + 1], real), above[32 * s + i] * upper]
        strip, far_strip = masked(strip, real), far_strip * upper
        edge = [rolled(strip, 120 - base, 1), rolled(strip, 88 - base, 1), rolled(far_strip, 120 - at, 1)]
        after = [jnp.where(lane == 127, edge[t], rolled(main[t], -1, 1)) for t in range(3)]
        both = [after[t] + main[t] for t in range(3)]
        change = [after[t] - main[t] for t in range(3)]

        def follow(v):
            turned = [rolled(t, -1, 0) for t in v]
            return [jnp.where(row == 7, turned[t + 1], turned[t]) for t in range(2)]

        both_next, change_next = follow(both), follow(change)
        join2 = lambda v: jnp.concatenate(v[:2], axis=0)
        both, change, both_next, change_next = join2(both), join2(change), join2(both_next), join2(change_next)
        return both_next + both, both_next - both, change_next + change

    scores = []
    old = [node(c, 0) for c in range(3)]
    for x in range(8):
        new = [node(c, x + 1) for c in range(3)]
        values = scaled_stress(strain_of(new, old), 0.25 * shear_modulus)
        old = new
        dens = mid[48 + 2 * x : 50 + 2 * x].reshape(BY, 128)
        scores.append(power_scale * jnp.sqrt(dens * mises(values) + 1.0))
    most = functools.reduce(jnp.maximum, scores)
    top = jnp.max(most, axis=(0, 1), keepdims=True)
    total = sum(jnp.exp(score - top) for score in scores)
    total = jnp.sum(total, axis=(0, 1), keepdims=True)
    stats[0] = jnp.broadcast_to(top, (8, 128))
    stats[1] = jnp.broadcast_to(total, (8, 128))


def beside(body, ins, outs):
    def run(*refs):
        refs[ins + 1 + outs][...] = refs[ins][...]
        body(*refs[:ins], *refs[ins + 1 : ins + 1 + outs], *refs[ins + 2 + outs :])

    return run


def widen_kernel(mid, low, high, far, below, above, disp, line, edge, cells):
    sources = (low, mid, high)
    for p in range(NODES):
        for c in range(4 if p < CELLS else 3):
            value, beyond = unpacked(c, p, sources, far, below, above)
            if c == 3:
                cells[p] = value
            else:
                disp[c, p] = value
                line[c, p] = beyond[0]
                edge[c, p] = beyond[1]


def stress_kernel(disp, line, edge, cells, base, stress, highest, corners):
    def planes(p):
        return [corner_sums(disp[c, p], (line[c, p], edge[c, p])) for c in range(3)]

    put_corners(corners, planes(0))
    highest[...] = jnp.zeros((ROWS, 128), F32)

    def step(p, n):
        news = [get_corners(corners)] + [planes(p + 1 + j) for j in range(n)]
        most = highest[...]
        for j in range(n):
            values = scaled_stress(strain_of(news[j + 1], news[j]), 0.25 * shear_modulus)
            dens = cells[p + j]
            for i in range(6):
                base[i, p + j] = values[i]
            local = jnp.sqrt(dens * mises(values) + 1.0)
            stress[p + j] = local
            most = jnp.maximum(most, jnp.where(dens > 0.0, local, 0.0))
        highest[...] = most
        put_corners(corners, news[n])

    in_groups(0, CELLS, 2, step)


def load_kernel(base, cells, stress, highest, rhs, stiff, weight, explicit, field, reference, held, kept):
    top = power_scale * jnp.max(highest[...], axis=(0, 1), keepdims=True)
    reference[...] = jnp.broadcast_to(top, (8, 128))

    def element(p):
        dens = cells[p]
        values = [base[i, p] for i in range(6)]
        local = stress[p]
        factor = jnp.where(dens > 0.0, jnp.exp(power_scale * local - top), 0.0) / (2.0 * local)
        explicit[p] = factor * mises(values)
        part = scaled_stress(mises_slope(values), (0.25 * shear_modulus) * dens * factor)
        rigid = jnp.where(dens > 0.0, 0.01 + 0.99 * (dens * dens * dens), 0.0)
        stiff[p] = (shear_modulus / 16.0) * rigid
        return part, rigid

    part, rigid = element(0)
    for i in range(6):
        held[i] = part[i]
    kept[...] = rigid
    for c in range(3):
        field[c, 0] = jnp.zeros((ROWS, 128), F32)
        field[c, CELLS] = jnp.zeros((ROWS, 128), F32)

    def step(p, n):
        parts = [([held[i] for i in range(6)], kept[...])] + [element(p + j) for j in range(n)]
        for i in range(6):
            held[i] = parts[n][0][i]
        kept[...] = parts[n][1]
        for j in range(n):
            load = forces(parts[j][0], parts[j + 1][0])
            total = parts[j][1] + parts[j + 1][1]
            total = total + y_prev(total)
            total = total + z_prev(total)
            own = jnp.where(cells[p + j] > 0.0, damping / (diag_factor * total + shift_term), 0.0)
            weight[p + j] = own
            for c in range(3):
                value = own * load[c]
                rhs[c, p + j] = value
                field[c, p + j] = value

    in_groups(1, CELLS, GROUP, step)


def sweep_kernel(lo, hi, start, rhs, stiff, weight, field, held, corners):
    def planes(p):
        return [corner_sums(v) for v in get3(start, p)]

    def element(new, old, p):
        return scaled_stress(strain_of(new, old), stiff[p])

    first, second = planes(lo - 1), planes(lo)
    part = element(second, first, lo - 1)
    for i in range(6):
        held[i] = part[i]
    put_corners(corners, second)

    def step(p, n):
        news = [get_corners(corners)] + [planes(p + 1 + j) for j in range(n)]
        put_corners(corners, news[n])
        part = [held[i] for i in range(6)]
        for j in range(n):
            here = element(news[j + 1], news[j], p + j)
            force = forces(part, here)
            part = here
            own = weight[p + j]
            keep = 1.0 - shift_term * own
            for c in range(3):
                field[c, p + j] = keep * start[c, p + j] + rhs[c, p + j] - own * force[c]
        for i in range(6):
            held[i] = part[i]

    count = -(-(hi + 1 - lo) // GROUP) * GROUP
    in_groups(lo, lo + count, GROUP, step)


def positions(axis, length, cell):
    whole = lax.axis_size(axis) * length
    place = lax.axis_index(axis) * length + cell
    return lambda o: ((place + o >= 0) & (place + o < whole)).astype(F32)


def final_kernel(field, explicit, base, cells, reference, everyone, adjoint, sens, aggregate, corners, near, side, out):
    elements = BX * BY * BZ * lax.axis_size("gx") * lax.axis_size("gy") * lax.axis_size("gz")
    top, total = everyone[0], everyone[1]
    scale = jnp.exp(reference[...] - top) / total * float(elements)
    aggregate[...] = ((top + jnp.log(total)) / power_scale)[0:1, 0:1]
    scale = jnp.broadcast_to(scale[0:1, 0:1], (BY, 128))
    for c in range(3):
        for p in range(8):
            adjoint[c, p] = scale * field[c, 8 + p, 8:24, :]

    row = lax.broadcasted_iota(jnp.int32, (ROWS, 128), 0)
    lane = lax.broadcasted_iota(jnp.int32, (ROWS, 128), 1)
    group, place = lane // 32, lane % 32
    main = row < 32
    y_cell = jnp.where(main, row - 8, 8 * group + row - 40)
    z_cell = jnp.where(main, lane, jnp.where(place < 16, 121 + place, place - 24))
    in_y, in_z = positions("gy", BY, y_cell), positions("gz", BZ, z_cell)
    ys, zs = {o: in_y(o) for o in range(-2, 3)}, {o: in_z(o) for o in range(-2, 3)}
    beside = ys[-1] + ys[1]
    across = zs[-1] + zs[1]
    ones = beside * zs[0] + ys[0] * across
    diagonal = beside * across
    twos = (ys[-2] + ys[2]) * zs[0] + ys[0] * (zs[-2] + zs[2])
    centre = ys[0] * zs[0]
    near_0 = 2.5 * centre + W1 * ones + W2 * diagonal + W4 * twos
    near_1 = W1 * centre + W2 * ones + W3 * diagonal
    near_2 = W4 * centre

    def planes(p):
        return [corner_sums(v) for v in get3(field, p)]

    put_corners(corners, planes(6))

    def step(p, n):
        news = [get_corners(corners)] + [planes(p + 1 + j) for j in range(n)]
        put_corners(corners, news[n])
        for j in range(n):
            q = p + j
            strain = strain_of(news[j + 1], news[j])
            dens = cells[q]
            worked = base[0, q] * strain[0]
            for i in range(1, 6):
                worked = worked + base[i, q] * strain[i]
            raw = explicit[q] - (0.25 * 2.97) * dens * dens * worked
            in_x = positions("gx", BX, q - 8)
            hsum = near_0 + near_1 * (in_x(-1) + in_x(1)) + near_2 * (in_x(-2) + in_x(2))
            value = jnp.where(dens > 0.0, raw / jnp.where(dens > 0.0, hsum, 1.0), 0.0)
            above, under = z_next(value), z_prev(value)
            left, right = y_next(value), y_prev(value)
            row_pair = above + under
            unit = row_pair + (left + right)
            corner = y_next(row_pair) + y_prev(row_pair)
            two = z_next(above) + z_prev(under) + y_next(left) + y_prev(right)
            near[q - 6] = (2.5 * value + W1 * unit + W2 * corner + W4 * two)[8:24]
            side[q - 6] = (W1 * value + W2 * unit + W3 * corner)[8:24]
            out[q - 6] = (W4 * value)[8:24]

    in_groups(6, 18, GROUP, step)
    for p in range(8):
        q = p + 2
        sens[p] = scale * (near[q] + (side[q - 1] + side[q + 1]) + (out[q - 2] + out[q + 2]))


def passed(block, axis, distance):
    count = lax.axis_size(axis)
    return lax.ppermute(block, axis, [(i, (i + distance) % count) for i in range(count)])


def within(axis, distance):
    place = lax.axis_index(axis) + distance
    return ((place >= 0) & (place < lax.axis_size(axis))).astype(F32)


def merged(mine, other):
    larger = jnp.maximum(mine[0], other[0])
    gap = jnp.exp(jnp.minimum(mine[0], other[0]) - larger)
    first = mine[0] >= other[0]
    total = jnp.where(first, mine[1], other[1]) + jnp.where(first, other[1], mine[1]) * gap
    return jnp.stack([larger, total])


def on_device(displacement, density):
    plane = (ROWS, 128)
    main = jnp.concatenate([displacement.reshape(48, 8, 128), density.reshape(16, 8, 128)], axis=0)
    up, down, inner, first = kernel_call(pack_z, [(16, 8, 128)] * 3 + [(6, 8, 128)], "pack_z")(main)
    below_z, above_z = passed(up, "gz", 1), passed(down, "gz", -1)
    strips = inner + below_z * within("gz", -1) + above_z * within("gz", 1)
    mid = jnp.concatenate([main, strips], axis=0)
    far = jnp.concatenate([first, strips[0:1], strips[4:5], strips[8:9]], axis=0)
    low, high, far = passed(mid, "gx", 1), passed(mid, "gx", -1), passed(far, "gx", -2)
    up, down = kernel_call(pack_y, [(126, 8, 128), (141, 8, 128)], "pack_y")(mid, low, high, far)
    below, above = passed(up, "gy", 1), passed(down, "gy", -1)
    (known,) = kernel_call(own_kernel, [(2, 8, 128)], "own")(mid, high, above, below)
    rounds = iter([("gy", 1), ("gy", 2), ("gy", 4), ("gx", 1), ("gx", 2), ("gx", 4), ("gz", 1), ("gz", 2)])

    def under(body, outs, name, scratch, aliases=None):
        def run(*args):
            nonlocal known
            axis, hop = next(rounds)
            other = lax.ppermute(known, axis, [(i, i ^ hop) for i in range(lax.axis_size(axis))])
            shapes = [*outs, (2, 8, 128)]
            call = kernel_call(beside(body, len(args), len(outs)), shapes, name, scratch, BUSY, aliases)
            *result, mine = call(*args, known)
            known = merged(mine, other)
            return result

        return run

    disp, line, edge, cells = under(
        widen_kernel,
        [(3, NODES, *plane), (3, NODES, 8, 128), (3, NODES, 8, 128), (CELLS, *plane)],
        "widen",
        [],
    )(mid, low, high, far, below, above)
    base, stress, highest = under(
        stress_kernel,
        [(6, CELLS, *plane), (CELLS, *plane), plane],
        "stress",
        [pltpu.VMEM((9, *plane), F32)],
    )(disp, line, edge, cells)
    rhs, stiff, weight, explicit, field, reference = under(
        load_kernel,
        [(3, CELLS, *plane), (CELLS, *plane), (CELLS, *plane), (CELLS, *plane), (3, NODES, *plane), (8, 128)],
        "load",
        [pltpu.VMEM((6, *plane), F32), pltpu.VMEM(plane, F32)],
    )(base, cells, stress, highest)
    for k in range(1, ITERS):
        (field,) = under(
            functools.partial(sweep_kernel, 1 + k, 23 - k),
            [(3, NODES, *plane)],
            f"sweep{k}",
            [pltpu.VMEM((6, *plane), F32), pltpu.VMEM((9, *plane), F32)],
            {0: 0},
        )(field, rhs, stiff, weight)
    everyone = known
    adjoint, sens, aggregate = kernel_call(
        final_kernel,
        [(3, BX, BY, BZ), (BX, BY, BZ), (1, 1)],
        "final",
        [
            pltpu.VMEM((9, *plane), F32),
            pltpu.VMEM((12, BY, 128), F32),
            pltpu.VMEM((12, BY, 128), F32),
            pltpu.VMEM((12, BY, 128), F32),
        ],
    )(field, explicit, base, cells, reference, everyone)
    return aggregate.reshape(()), adjoint, sens


def solution(mesh):
    placed = (P(None, "gx", "gy", "gz"), P("gx", "gy", "gz"))
    return jax.shard_map(
        on_device,
        mesh=mesh,
        in_specs=placed,
        out_specs=(P(), P(None, "gx", "gy", "gz"), P("gx", "gy", "gz")),
        check_vma=False,
    )
```

```python
import functools
import math

import jax
import jax.numpy as jnp
from jax import lax
from jax.experimental import pallas as pl
from jax.experimental.pallas import tpu as pltpu
from jax.sharding import PartitionSpec as P

ITERS = 6
lame_first = 0.3 / (1.3 * 0.4)
shear_modulus = 1.0 / 2.6
lame_ratio = lame_first / shear_modulus
power_scale = 3.0
damping = 0.6
shift_term = 0.1
diag_factor = (lame_first + 3.0 * shear_modulus) / 16.0
W1, W2, W3 = (2.5 - math.sqrt(n) for n in (1, 2, 3))
W4 = 0.5
AXES = ("gx", "gy", "gz")

BX, BY, BZ = 8, 16, 128
NODES, CELLS = 25, 24
ROWS = 40
F32 = jnp.float32
VM = 24 * 1024 * 1024
GROUP = 3
BUSY = 20_000_000


def tile(value):
    return jax.ShapeDtypeStruct(value, F32)


def kernel_call(body, outs, name, scratch=(), flops=1_000_000, aliases=None):
    spec = pl.BlockSpec(memory_space=pltpu.VMEM)

    def run(*args):
        return pl.pallas_call(
            body,
            out_shape=[tile(shape) for shape in outs],
            in_specs=[spec] * len(args),
            out_specs=[spec] * len(outs),
            scratch_shapes=list(scratch),
            input_output_aliases=aliases or {},
            name=name,
            compiler_params=pltpu.CompilerParams(vmem_limit_bytes=VM),
            cost_estimate=pl.CostEstimate(flops=flops, bytes_accessed=1_000_000, transcendentals=0),
        )(*args)

    return run


def rolled(value, shift, axis):
    shift = shift % value.shape[axis]
    return value if shift == 0 else pltpu.roll(value, shift, axis)


def lanes():
    return lax.broadcasted_iota(jnp.int32, (8, 128), 1)


def rows():
    return lax.broadcasted_iota(jnp.int32, (8, 128), 0)


def split(value):
    return [value[8 * g : 8 * g + 8] for g in range(4)], value[32:40]


def join(main, strip):
    return jnp.concatenate([*main, strip], axis=0)


def z_next(value):
    main, strip = split(value)
    last = lanes() == 127
    out = [jnp.where(last, rolled(strip, 120 - 32 * g, 1), rolled(main[g], -1, 1)) for g in range(4)]
    return join(out, rolled(strip, -1, 1))


def z_prev(value):
    main, strip = split(value)
    first = lanes() == 0
    out = [jnp.where(first, rolled(strip, -23 - 32 * g, 1), rolled(main[g], 1, 1)) for g in range(4)]
    return join(out, rolled(strip, 1, 1))


def y_next(value, beyond=None):
    main, strip = split(value)
    row = rows()
    turned = [rolled(m, -1, 0) for m in main]
    follow = [turned[1], turned[2], turned[3], turned[3] if beyond is None else beyond[0]]
    out = [jnp.where(row == 7, follow[g], turned[g]) for g in range(4)]
    tail = rolled(strip, -1, 0)
    after = rolled(tail, -32, 1)
    if beyond is not None:
        after = jnp.where(lanes() >= 96, beyond[1], after)
    return join(out, jnp.where(row == 7, after, tail))


def y_prev(value):
    main, strip = split(value)
    row = rows()
    turned = [rolled(m, 1, 0) for m in main]
    before = [turned[0], turned[0], turned[1], turned[2]]
    out = [jnp.where(row == 0, before[g], turned[g]) for g in range(4)]
    tail = rolled(strip, 1, 0)
    return join(out, jnp.where(row == 0, rolled(tail, 32, 1), tail))


def pack_z(main, up, down, inner, first):
    lane = lanes()
    for c in range(4):
        short = 0 if c < 3 else 1
        for k in range(4):
            top = bottom = own = jnp.zeros((8, 128), F32)
            for q in range(4):
                value = main[16 * c + 2 * (k + 4 * (q // 2)) + q % 2]
                place = lane - 32 * q
                top = jnp.where((place >= 16) & (place < 24), rolled(value, 32 * q + 24, 1), top)
                bottom = jnp.where((place >= 7) & (place < 16 - short), rolled(value, 32 * q + 7, 1), bottom)
                own = jnp.where((place >= 24) & (place < 32 - short), rolled(value, 32 * q + 24, 1), own)
                own = jnp.where((place >= 0) & (place < 7), rolled(value, 32 * q + 7, 1), own)
            if k == 0 and c < 3:
                first[2 * c] = main[16 * c]
                first[2 * c + 1] = main[16 * c + 1]
            up[4 * c + k] = top
            down[4 * c + k] = bottom
            inner[4 * c + k] = own


def masked(value, real):
    return value if real is None else value * real


def pack_y(mid, low, high, far, up, down):
    lane = lanes()
    odd = (lane // 32) % 2 == 1
    sources = (low, mid, high)
    for s, src in enumerate(sources):
        real = None if s == 1 else within("gx", s - 1)
        for i in range(32):
            up[32 * s + i] = masked(src[2 * i + 1], real)
            down[32 * s + i] = masked(src[2 * i], real)
        for c in range(4):
            for k in range(2):
                first, second = src[64 + 4 * c + k], src[64 + 4 * c + k + 2]
                up[99 + 8 * s + 2 * c + k] = masked(jnp.where(odd, first, rolled(second, -32, 1)), real)
                down[99 + 8 * s + 2 * c + k] = masked(jnp.where(odd, rolled(second, 32, 1), first), real)
        for i in range(24):
            r = 24 * s + i
            down[126 + r // 8, r % 8 : r % 8 + 1, :] = masked(src[2 * i + 1, 0:1, :], real)
        for i in range(12):
            r = 12 * s + i
            down[136 + r // 8, r % 8 : r % 8 + 1, :] = masked(src[64 + i, 0:1, :], real)
    real = within("gx", 2)
    for c in range(3):
        up[96 + c] = masked(far[2 * c + 1], real)
        down[96 + c] = masked(far[2 * c], real)
        up[123 + c] = masked(far[6 + c], real)
        down[123 + c] = masked(far[6 + c], real)
        r = 72 + c
        down[126 + r // 8, r % 8 : r % 8 + 1, :] = masked(far[2 * c + 1, 0:1, :], real)
        r = 36 + c
        down[136 + r // 8, r % 8 : r % 8 + 1, :] = masked(far[6 + c, 0:1, :], real)


def unpacked(c, p, sources, far, below, above):
    lane = lanes()
    group = lane // 32
    real = (within("gx", -1), None, within("gx", 1), within("gx", 2))[p // 8]
    lower, upper = within("gy", -1), within("gy", 1)
    if p < 24:
        s, x = divmod(p, 8)
        src, i, k = sources[s], 8 * c + x, x % 4
        own = rolled(src[64 + 4 * c + k], 32 if x < 4 else -32, 1)
        slot = 99 + 8 * s + 2 * c + x % 2
        under = rolled(below[slot], {0: -32, 1: -96, 2: 0, 3: -64}[(1 if x >= 4 else 0) + (2 if k >= 2 else 0)], 1)
        over = rolled(above[slot], {0: 96, 1: 32, 2: 64, 3: 0}[(1 if x >= 4 else 0) + (2 if k >= 2 else 0)], 1)
        main = [below[32 * s + i], src[2 * i], src[2 * i + 1], above[32 * s + i]]
        r, q = 24 * s + i, 12 * s + 4 * c + k
        turn = 64 if x < 4 else 0
    else:
        own = rolled(far[6 + c], 32, 1)
        under = rolled(below[123 + c], -32, 1)
        over = rolled(above[123 + c], 96, 1)
        main = [below[96 + c], far[2 * c], far[2 * c + 1], above[96 + c]]
        r, q, turn = 72 + c, 36 + c, 64
    main = [main[0] * lower, masked(main[1], real), masked(main[2], real), main[3] * upper]
    strip = jnp.where(group == 0, under * lower, jnp.where(group == 3, over * upper, masked(own, real)))
    if c == 3:
        return join(main, strip), None
    line = jnp.broadcast_to(above[126 + r // 8, r % 8 : r % 8 + 1, :], (8, 128))
    edge = jnp.broadcast_to(above[136 + q // 8, q % 8 : q % 8 + 1, :], (8, 128))
    return join(main, strip), (line * upper, rolled(edge, turn, 1) * upper)


def corner_sums(value, beyond=None):
    if beyond is not None:
        following = y_next(value, beyond)
        both, change = following + value, following - value
        first, second = z_next(both), z_next(change)
        return first + both, second + change, first - both
    following = z_next(value)
    both, change = following + value, following - value
    after = y_next(both)
    return after + both, after - both, y_next(change) + change


def strain_of(new, old):
    grad = [[new[c][0] - old[c][0] for c in range(3)]]
    grad.append([new[c][1] + old[c][1] for c in range(3)])
    grad.append([new[c][2] + old[c][2] for c in range(3)])
    return [
        grad[0][0],
        grad[1][1],
        grad[2][2],
        grad[0][1] + grad[1][0],
        grad[1][2] + grad[2][1],
        grad[2][0] + grad[0][2],
    ]


def scaled_stress(values, factor):
    trace = lame_ratio * (values[0] + values[1] + values[2])
    return [factor * (trace + 2.0 * v) for v in values[:3]] + [factor * v for v in values[3:]]


def forces(prev, here):
    add = [prev[i] + here[i] for i in range(6)]
    sub = {i: prev[i] - here[i] for i in (0, 3, 5)}
    out = []
    for along_x, along_y, along_z in ((0, 3, 5), (3, 1, 4), (5, 4, 2)):
        a, b, w = sub[along_x], add[along_y], add[along_z]
        first = y_prev(a + b) + (a - b)
        second = y_prev(w) + w
        out.append(z_prev(first + second) + (first - second))
    return out


def get3(ref, p):
    return [ref[c, p] for c in range(3)]


def put_corners(ref, values):
    for c in range(3):
        for i in range(3):
            ref[3 * c + i] = values[c][i]


def get_corners(ref):
    return [[ref[3 * c + i] for i in range(3)] for c in range(3)]


def mises(v):
    return (
        v[0] * v[0] + v[1] * v[1] + v[2] * v[2] - v[0] * v[1] - v[1] * v[2] - v[2] * v[0]
        + 3.0 * (v[3] * v[3] + v[4] * v[4] + v[5] * v[5])
    )


def mises_slope(v):
    return [
        2.0 * v[0] - v[1] - v[2],
        2.0 * v[1] - v[2] - v[0],
        2.0 * v[2] - v[0] - v[1],
        6.0 * v[3],
        6.0 * v[4],
        6.0 * v[5],
    ]


def in_groups(lo, hi, size, body):
    full = (hi - lo) // size

    def step(i, carry):
        body(lo + size * i, size)
        return carry

    if full:
        lax.fori_loop(0, full, step, 0)
    if lo + size * full < hi:
        body(lo + size * full, hi - lo - size * full)


def own_kernel(mid, high, above, below, stats):
    lane = lanes()
    row = rows()

    def node(c, x):
        src, i, k = (mid, 8 * c + x, x % 4) if x < 8 else (high, 8 * c, 0)
        s = 1 if x < 8 else 2
        x = x % 8
        strip = src[64 + 4 * c + k]
        base = 64 if x >= 4 else 0
        far_strip = above[99 + 8 * s + 2 * c + x % 2]
        at = 64 * (x // 4) + (32 if k >= 2 else 0)
        real = None if s == 1 else within("gx", 1)
        upper = within("gy", 1)
        main = [masked(src[2 * i], real), masked(src[2 * i + 1], real), above[32 * s + i] * upper]
        strip, far_strip = masked(strip, real), far_strip * upper
        edge = [rolled(strip, 120 - base, 1), rolled(strip, 88 - base, 1), rolled(far_strip, 120 - at, 1)]
        after = [jnp.where(lane == 127, edge[t], rolled(main[t], -1, 1)) for t in range(3)]
        both = [after[t] + main[t] for t in range(3)]
        change = [after[t] - main[t] for t in range(3)]

        def follow(v):
            turned = [rolled(t, -1, 0) for t in v]
            return [jnp.where(row == 7, turned[t + 1], turned[t]) for t in range(2)]

        both_next, change_next = follow(both), follow(change)
        join2 = lambda v: jnp.concatenate(v[:2], axis=0)
        both, change, both_next, change_next = join2(both), join2(change), join2(both_next), join2(change_next)
        return both_next + both, both_next - both, change_next + change

    scores = []
    old = [node(c, 0) for c in range(3)]
    for x in range(8):
        new = [node(c, x + 1) for c in range(3)]
        values = scaled_stress(strain_of(new, old), 0.25 * shear_modulus)
        old = new
        dens = mid[48 + 2 * x : 50 + 2 * x].reshape(BY, 128)
        scores.append(power_scale * jnp.sqrt(dens * mises(values) + 1.0))
    most = functools.reduce(jnp.maximum, scores)
    top = jnp.max(most, axis=(0, 1), keepdims=True)
    total = sum(jnp.exp(score - top) for score in scores)
    total = jnp.sum(total, axis=(0, 1), keepdims=True)
    stats[0] = jnp.broadcast_to(top, (8, 128))
    stats[1] = jnp.broadcast_to(total, (8, 128))


def beside(body, ins, outs):
    def run(*refs):
        refs[ins + 1 + outs][...] = refs[ins][...]
        body(*refs[:ins], *refs[ins + 1 : ins + 1 + outs], *refs[ins + 2 + outs :])

    return run


def widen_kernel(mid, low, high, far, below, above, disp, line, edge, cells):
    sources = (low, mid, high)
    for p in range(NODES):
        for c in range(4 if p < CELLS else 3):
            value, beyond = unpacked(c, p, sources, far, below, above)
            if c == 3:
                cells[p] = value
            else:
                disp[c, p] = value
                line[c, p] = beyond[0]
                edge[c, p] = beyond[1]


def stress_kernel(disp, line, edge, cells, base, stress, highest, corners):
    def planes(p):
        return [corner_sums(disp[c, p], (line[c, p], edge[c, p])) for c in range(3)]

    put_corners(corners, planes(0))
    highest[...] = jnp.zeros((ROWS, 128), F32)

    def step(p, n):
        news = [get_corners(corners)] + [planes(p + 1 + j) for j in range(n)]
        most = highest[...]
        for j in range(n):
            values = scaled_stress(strain_of(news[j + 1], news[j]), 0.25 * shear_modulus)
            dens = cells[p + j]
            for i in range(6):
                base[i, p + j] = values[i]
            local = jnp.sqrt(dens * mises(values) + 1.0)
            stress[p + j] = local
            most = jnp.maximum(most, jnp.where(dens > 0.0, local, 0.0))
        highest[...] = most
        put_corners(corners, news[n])

    in_groups(0, CELLS, 2, step)


def load_kernel(base, cells, stress, highest, rhs, stiff, weight, explicit, field, reference, held, kept):
    top = power_scale * jnp.max(highest[...], axis=(0, 1), keepdims=True)
    reference[...] = jnp.broadcast_to(top, (8, 128))

    def element(p):
        dens = cells[p]
        values = [base[i, p] for i in range(6)]
        local = stress[p]
        factor = jnp.where(dens > 0.0, jnp.exp(power_scale * local - top), 0.0) / (2.0 * local)
        explicit[p] = factor * mises(values)
        part = scaled_stress(mises_slope(values), (0.25 * shear_modulus) * dens * factor)
        rigid = jnp.where(dens > 0.0, 0.01 + 0.99 * (dens * dens * dens), 0.0)
        stiff[p] = (shear_modulus / 16.0) * rigid
        return part, rigid

    part, rigid = element(0)
    for i in range(6):
        held[i] = part[i]
    kept[...] = rigid
    for c in range(3):
        field[c, 0] = jnp.zeros((ROWS, 128), F32)
        field[c, CELLS] = jnp.zeros((ROWS, 128), F32)

    def step(p, n):
        parts = [([held[i] for i in range(6)], kept[...])] + [element(p + j) for j in range(n)]
        for i in range(6):
            held[i] = parts[n][0][i]
        kept[...] = parts[n][1]
        for j in range(n):
            load = forces(parts[j][0], parts[j + 1][0])
            total = parts[j][1] + parts[j + 1][1]
            total = total + y_prev(total)
            total = total + z_prev(total)
            own = jnp.where(cells[p + j] > 0.0, damping / (diag_factor * total + shift_term), 0.0)
            weight[p + j] = own
            for c in range(3):
                value = own * load[c]
                rhs[c, p + j] = value
                field[c, p + j] = value

    in_groups(1, CELLS, GROUP, step)


def sweep_kernel(lo, hi, start, rhs, stiff, weight, field, held, corners):
    def planes(p):
        return [corner_sums(v) for v in get3(start, p)]

    def element(new, old, p):
        return scaled_stress(strain_of(new, old), stiff[p])

    first, second = planes(lo - 1), planes(lo)
    part = element(second, first, lo - 1)
    for i in range(6):
        held[i] = part[i]
    put_corners(corners, second)

    def step(p, n):
        news = [get_corners(corners)] + [planes(p + 1 + j) for j in range(n)]
        put_corners(corners, news[n])
        part = [held[i] for i in range(6)]
        for j in range(n):
            here = element(news[j + 1], news[j], p + j)
            force = forces(part, here)
            part = here
            own = weight[p + j]
            keep = 1.0 - shift_term * own
            for c in range(3):
                field[c, p + j] = keep * start[c, p + j] + rhs[c, p + j] - own * force[c]
        for i in range(6):
            held[i] = part[i]

    count = -(-(hi + 1 - lo) // GROUP) * GROUP
    in_groups(lo, lo + count, GROUP, step)


def positions(axis, length, cell):
    whole = lax.axis_size(axis) * length
    place = lax.axis_index(axis) * length + cell
    return lambda o: ((place + o >= 0) & (place + o < whole)).astype(F32)


def final_kernel(field, explicit, base, cells, reference, everyone, adjoint, sens, aggregate, corners, near, side, out):
    elements = BX * BY * BZ * lax.axis_size("gx") * lax.axis_size("gy") * lax.axis_size("gz")
    top, total = everyone[0], everyone[1]
    scale = jnp.exp(reference[...] - top) / total * float(elements)
    aggregate[...] = ((top + jnp.log(total)) / power_scale)[0:1, 0:1]
    scale = jnp.broadcast_to(scale[0:1, 0:1], (BY, 128))
    for c in range(3):
        for p in range(8):
            adjoint[c, p] = scale * field[c, 8 + p, 8:24, :]

    row = lax.broadcasted_iota(jnp.int32, (ROWS, 128), 0)
    lane = lax.broadcasted_iota(jnp.int32, (ROWS, 128), 1)
    group, place = lane // 32, lane % 32
    main = row < 32
    y_cell = jnp.where(main, row - 8, 8 * group + row - 40)
    z_cell = jnp.where(main, lane, jnp.where(place < 16, 121 + place, place - 24))
    in_y, in_z = positions("gy", BY, y_cell), positions("gz", BZ, z_cell)
    ys, zs = {o: in_y(o) for o in range(-2, 3)}, {o: in_z(o) for o in range(-2, 3)}
    beside = ys[-1] + ys[1]
    across = zs[-1] + zs[1]
    ones = beside * zs[0] + ys[0] * across
    diagonal = beside * across
    twos = (ys[-2] + ys[2]) * zs[0] + ys[0] * (zs[-2] + zs[2])
    centre = ys[0] * zs[0]
    near_0 = 2.5 * centre + W1 * ones + W2 * diagonal + W4 * twos
    near_1 = W1 * centre + W2 * ones + W3 * diagonal
    near_2 = W4 * centre

    def planes(p):
        return [corner_sums(v) for v in get3(field, p)]

    put_corners(corners, planes(6))

    def step(p, n):
        news = [get_corners(corners)] + [planes(p + 1 + j) for j in range(n)]
        put_corners(corners, news[n])
        for j in range(n):
            q = p + j
            strain = strain_of(news[j + 1], news[j])
            dens = cells[q]
            worked = base[0, q] * strain[0]
            for i in range(1, 6):
                worked = worked + base[i, q] * strain[i]
            raw = explicit[q] - (0.25 * 2.97) * dens * dens * worked
            in_x = positions("gx", BX, q - 8)
            hsum = near_0 + near_1 * (in_x(-1) + in_x(1)) + near_2 * (in_x(-2) + in_x(2))
            value = jnp.where(dens > 0.0, raw / jnp.where(dens > 0.0, hsum, 1.0), 0.0)
            above, under = z_next(value), z_prev(value)
            left, right = y_next(value), y_prev(value)
            row_pair = above + under
            unit = row_pair + (left + right)
            corner = y_next(row_pair) + y_prev(row_pair)
            two = z_next(above) + z_prev(under) + y_next(left) + y_prev(right)
            near[q - 6] = (2.5 * value + W1 * unit + W2 * corner + W4 * two)[8:24]
            side[q - 6] = (W1 * value + W2 * unit + W3 * corner)[8:24]
            out[q - 6] = (W4 * value)[8:24]

    in_groups(6, 18, GROUP, step)
    for p in range(8):
        q = p + 2
        sens[p] = scale * (near[q] + (side[q - 1] + side[q + 1]) + (out[q - 2] + out[q + 2]))


def passed(block, axis, distance):
    count = lax.axis_size(axis)
    return lax.ppermute(block, axis, [(i, (i + distance) % count) for i in range(count)])


def within(axis, distance):
    place = lax.axis_index(axis) + distance
    return ((place >= 0) & (place < lax.axis_size(axis))).astype(F32)


def merged(mine, other):
    larger = jnp.maximum(mine[0], other[0])
    gap = jnp.exp(jnp.minimum(mine[0], other[0]) - larger)
    first = mine[0] >= other[0]
    total = jnp.where(first, mine[1], other[1]) + jnp.where(first, other[1], mine[1]) * gap
    return jnp.stack([larger, total])


def on_device(displacement, density):
    plane = (ROWS, 128)
    main = jnp.concatenate([displacement.reshape(48, 8, 128), density.reshape(16, 8, 128)], axis=0)
    main = lax.optimization_barrier(main)
    up, down, inner, first = kernel_call(pack_z, [(16, 8, 128)] * 3 + [(6, 8, 128)], "pack_z")(main)
    below_z, above_z = passed(up, "gz", 1), passed(down, "gz", -1)
    strips = inner + below_z * within("gz", -1) + above_z * within("gz", 1)
    mid = jnp.concatenate([main, strips], axis=0)
    far = jnp.concatenate([first, strips[0:1], strips[4:5], strips[8:9]], axis=0)
    low, high, far = passed(mid, "gx", 1), passed(mid, "gx", -1), passed(far, "gx", -2)
    up, down = kernel_call(pack_y, [(126, 8, 128), (141, 8, 128)], "pack_y")(mid, low, high, far)
    below, above = passed(up, "gy", 1), passed(down, "gy", -1)
    (known,) = kernel_call(own_kernel, [(2, 8, 128)], "own")(mid, high, above, below)
    rounds = iter([("gy", 1), ("gy", 2), ("gy", 4), ("gx", 1), ("gx", 2), ("gx", 4), ("gz", 1), ("gz", 2)])

    def under(body, outs, name, scratch, aliases=None):
        def run(*args):
            nonlocal known
            axis, hop = next(rounds)
            other = lax.ppermute(known, axis, [(i, i ^ hop) for i in range(lax.axis_size(axis))])
            shapes = [*outs, (2, 8, 128)]
            call = kernel_call(beside(body, len(args), len(outs)), shapes, name, scratch, BUSY, aliases)
            *result, mine = call(*args, known)
            known = merged(mine, other)
            return result

        return run

    disp, line, edge, cells = under(
        widen_kernel,
        [(3, NODES, *plane), (3, NODES, 8, 128), (3, NODES, 8, 128), (CELLS, *plane)],
        "widen",
        [],
    )(mid, low, high, far, below, above)
    base, stress, highest = under(
        stress_kernel,
        [(6, CELLS, *plane), (CELLS, *plane), plane],
        "stress",
        [pltpu.VMEM((9, *plane), F32)],
    )(disp, line, edge, cells)
    rhs, stiff, weight, explicit, field, reference = under(
        load_kernel,
        [(3, CELLS, *plane), (CELLS, *plane), (CELLS, *plane), (CELLS, *plane), (3, NODES, *plane), (8, 128)],
        "load",
        [pltpu.VMEM((6, *plane), F32), pltpu.VMEM(plane, F32)],
    )(base, cells, stress, highest)
    for k in range(1, ITERS):
        (field,) = under(
            functools.partial(sweep_kernel, 1 + k, 23 - k),
            [(3, NODES, *plane)],
            f"sweep{k}",
            [pltpu.VMEM((6, *plane), F32), pltpu.VMEM((9, *plane), F32)],
            {0: 0},
        )(field, rhs, stiff, weight)
    everyone = known
    adjoint, sens, aggregate = kernel_call(
        final_kernel,
        [(3, BX, BY, BZ), (BX, BY, BZ), (1, 1)],
        "final",
        [
            pltpu.VMEM((9, *plane), F32),
            pltpu.VMEM((12, BY, 128), F32),
            pltpu.VMEM((12, BY, 128), F32),
            pltpu.VMEM((12, BY, 128), F32),
        ],
    )(field, explicit, base, cells, reference, everyone)
    return aggregate.reshape(()), adjoint, sens


def solution(mesh):
    placed = (P(None, "gx", "gy", "gz"), P("gx", "gy", "gz"))
    return jax.shard_map(
        on_device,
        mesh=mesh,
        in_specs=placed,
        out_specs=(P(), P(None, "gx", "gy", "gz"), P("gx", "gy", "gz")),
        check_vma=False,
    )
```

```python
import functools
import math

import jax
import jax.numpy as jnp
from jax import lax
from jax.experimental import pallas as pl
from jax.experimental.pallas import tpu as pltpu
from jax.sharding import PartitionSpec as P

ITERS = 6
lame_first = 0.3 / (1.3 * 0.4)
shear_modulus = 1.0 / 2.6
lame_ratio = lame_first / shear_modulus
power_scale = 3.0
damping = 0.6
shift_term = 0.1
diag_factor = (lame_first + 3.0 * shear_modulus) / 16.0
W1, W2, W3 = (2.5 - math.sqrt(n) for n in (1, 2, 3))
W4 = 0.5
AXES = ("gx", "gy", "gz")

BX, BY, BZ = 8, 16, 128
NODES, CELLS = 25, 24
ROWS = 40
F32 = jnp.float32
VM = 24 * 1024 * 1024
GROUP = 3
BUSY = 20_000_000


def tile(value):
    return jax.ShapeDtypeStruct(value, F32)


def kernel_call(body, outs, name, scratch=(), flops=1_000_000, aliases=None):
    spec = pl.BlockSpec(memory_space=pltpu.VMEM)

    def run(*args):
        return pl.pallas_call(
            body,
            out_shape=[tile(shape) for shape in outs],
            in_specs=[spec] * len(args),
            out_specs=[spec] * len(outs),
            scratch_shapes=list(scratch),
            input_output_aliases=aliases or {},
            name=name,
            compiler_params=pltpu.CompilerParams(vmem_limit_bytes=VM),
            cost_estimate=pl.CostEstimate(flops=flops, bytes_accessed=1_000_000, transcendentals=0),
        )(*args)

    return run


def rolled(value, shift, axis):
    shift = shift % value.shape[axis]
    return value if shift == 0 else pltpu.roll(value, shift, axis)


def lanes():
    return lax.broadcasted_iota(jnp.int32, (8, 128), 1)


def rows():
    return lax.broadcasted_iota(jnp.int32, (8, 128), 0)


def split(value):
    return [value[8 * g : 8 * g + 8] for g in range(4)], value[32:40]


def join(main, strip):
    return jnp.concatenate([*main, strip], axis=0)


def z_next(value):
    main, strip = split(value)
    last = lanes() == 127
    out = [jnp.where(last, rolled(strip, 120 - 32 * g, 1), rolled(main[g], -1, 1)) for g in range(4)]
    return join(out, rolled(strip, -1, 1))


def z_prev(value):
    main, strip = split(value)
    first = lanes() == 0
    out = [jnp.where(first, rolled(strip, -23 - 32 * g, 1), rolled(main[g], 1, 1)) for g in range(4)]
    return join(out, rolled(strip, 1, 1))


def y_next(value, beyond=None):
    main, strip = split(value)
    row = rows()
    turned = [rolled(m, -1, 0) for m in main]
    follow = [turned[1], turned[2], turned[3], turned[3] if beyond is None else beyond[0]]
    out = [jnp.where(row == 7, follow[g], turned[g]) for g in range(4)]
    tail = rolled(strip, -1, 0)
    after = rolled(tail, -32, 1)
    if beyond is not None:
        after = jnp.where(lanes() >= 96, beyond[1], after)
    return join(out, jnp.where(row == 7, after, tail))


def y_prev(value):
    main, strip = split(value)
    row = rows()
    turned = [rolled(m, 1, 0) for m in main]
    before = [turned[0], turned[0], turned[1], turned[2]]
    out = [jnp.where(row == 0, before[g], turned[g]) for g in range(4)]
    tail = rolled(strip, 1, 0)
    return join(out, jnp.where(row == 0, rolled(tail, 32, 1), tail))


def pack_z(main, up, down, inner, first):
    lane = lanes()
    for c in range(4):
        short = 0 if c < 3 else 1
        for k in range(4):
            top = bottom = own = jnp.zeros((8, 128), F32)
            for q in range(4):
                value = main[16 * c + 2 * (k + 4 * (q // 2)) + q % 2]
                place = lane - 32 * q
                top = jnp.where((place >= 16) & (place < 24), rolled(value, 32 * q + 24, 1), top)
                bottom = jnp.where((place >= 7) & (place < 16 - short), rolled(value, 32 * q + 7, 1), bottom)
                own = jnp.where((place >= 24) & (place < 32 - short), rolled(value, 32 * q + 24, 1), own)
                own = jnp.where((place >= 0) & (place < 7), rolled(value, 32 * q + 7, 1), own)
            if k == 0 and c < 3:
                first[2 * c] = main[16 * c]
                first[2 * c + 1] = main[16 * c + 1]
            up[4 * c + k] = top
            down[4 * c + k] = bottom
            inner[4 * c + k] = own


def masked(value, real):
    return value if real is None else value * real


def pack_y(mid, low, high, far, up, down):
    lane = lanes()
    odd = (lane // 32) % 2 == 1
    sources = (low, mid, high)
    for s, src in enumerate(sources):
        real = None if s == 1 else within("gx", s - 1)
        for i in range(32):
            up[32 * s + i] = masked(src[2 * i + 1], real)
            down[32 * s + i] = masked(src[2 * i], real)
        for c in range(4):
            for k in range(2):
                first, second = src[64 + 4 * c + k], src[64 + 4 * c + k + 2]
                up[99 + 8 * s + 2 * c + k] = masked(jnp.where(odd, first, rolled(second, -32, 1)), real)
                down[99 + 8 * s + 2 * c + k] = masked(jnp.where(odd, rolled(second, 32, 1), first), real)
        for i in range(24):
            r = 24 * s + i
            down[126 + r // 8, r % 8 : r % 8 + 1, :] = masked(src[2 * i + 1, 0:1, :], real)
        for i in range(12):
            r = 12 * s + i
            down[136 + r // 8, r % 8 : r % 8 + 1, :] = masked(src[64 + i, 0:1, :], real)
    real = within("gx", 2)
    for c in range(3):
        up[96 + c] = masked(far[2 * c + 1], real)
        down[96 + c] = masked(far[2 * c], real)
        up[123 + c] = masked(far[6 + c], real)
        down[123 + c] = masked(far[6 + c], real)
        r = 72 + c
        down[126 + r // 8, r % 8 : r % 8 + 1, :] = masked(far[2 * c + 1, 0:1, :], real)
        r = 36 + c
        down[136 + r // 8, r % 8 : r % 8 + 1, :] = masked(far[6 + c, 0:1, :], real)


def unpacked(c, p, sources, far, below, above):
    lane = lanes()
    group = lane // 32
    real = (within("gx", -1), None, within("gx", 1), within("gx", 2))[p // 8]
    lower, upper = within("gy", -1), within("gy", 1)
    if p < 24:
        s, x = divmod(p, 8)
        src, i, k = sources[s], 8 * c + x, x % 4
        own = rolled(src[64 + 4 * c + k], 32 if x < 4 else -32, 1)
        slot = 99 + 8 * s + 2 * c + x % 2
        under = rolled(below[slot], {0: -32, 1: -96, 2: 0, 3: -64}[(1 if x >= 4 else 0) + (2 if k >= 2 else 0)], 1)
        over = rolled(above[slot], {0: 96, 1: 32, 2: 64, 3: 0}[(1 if x >= 4 else 0) + (2 if k >= 2 else 0)], 1)
        main = [below[32 * s + i], src[2 * i], src[2 * i + 1], above[32 * s + i]]
        r, q = 24 * s + i, 12 * s + 4 * c + k
        turn = 64 if x < 4 else 0
    else:
        own = rolled(far[6 + c], 32, 1)
        under = rolled(below[123 + c], -32, 1)
        over = rolled(above[123 + c], 96, 1)
        main = [below[96 + c], far[2 * c], far[2 * c + 1], above[96 + c]]
        r, q, turn = 72 + c, 36 + c, 64
    main = [main[0] * lower, masked(main[1], real), masked(main[2], real), main[3] * upper]
    strip = jnp.where(group == 0, under * lower, jnp.where(group == 3, over * upper, masked(own, real)))
    if c == 3:
        return join(main, strip), None
    line = jnp.broadcast_to(above[126 + r // 8, r % 8 : r % 8 + 1, :], (8, 128))
    edge = jnp.broadcast_to(above[136 + q // 8, q % 8 : q % 8 + 1, :], (8, 128))
    return join(main, strip), (line * upper, rolled(edge, turn, 1) * upper)


def corner_sums(value, beyond=None):
    if beyond is not None:
        following = y_next(value, beyond)
        both, change = following + value, following - value
        first, second = z_next(both), z_next(change)
        return first + both, second + change, first - both
    following = z_next(value)
    both, change = following + value, following - value
    after = y_next(both)
    return after + both, after - both, y_next(change) + change


def strain_of(new, old):
    grad = [[new[c][0] - old[c][0] for c in range(3)]]
    grad.append([new[c][1] + old[c][1] for c in range(3)])
    grad.append([new[c][2] + old[c][2] for c in range(3)])
    return [
        grad[0][0],
        grad[1][1],
        grad[2][2],
        grad[0][1] + grad[1][0],
        grad[1][2] + grad[2][1],
        grad[2][0] + grad[0][2],
    ]


def scaled_stress(values, factor):
    trace = lame_ratio * (values[0] + values[1] + values[2])
    return [factor * (trace + 2.0 * v) for v in values[:3]] + [factor * v for v in values[3:]]


def forces(prev, here):
    add = [prev[i] + here[i] for i in range(6)]
    sub = {i: prev[i] - here[i] for i in (0, 3, 5)}
    out = []
    for along_x, along_y, along_z in ((0, 3, 5), (3, 1, 4), (5, 4, 2)):
        a, b, w = sub[along_x], add[along_y], add[along_z]
        first = y_prev(a + b) + (a - b)
        second = y_prev(w) + w
        out.append(z_prev(first + second) + (first - second))
    return out


def get3(ref, p):
    return [ref[c, p] for c in range(3)]


def put_corners(ref, values):
    for c in range(3):
        for i in range(3):
            ref[3 * c + i] = values[c][i]


def get_corners(ref):
    return [[ref[3 * c + i] for i in range(3)] for c in range(3)]


def mises(v):
    return (
        v[0] * v[0] + v[1] * v[1] + v[2] * v[2] - v[0] * v[1] - v[1] * v[2] - v[2] * v[0]
        + 3.0 * (v[3] * v[3] + v[4] * v[4] + v[5] * v[5])
    )


def mises_slope(v):
    return [
        2.0 * v[0] - v[1] - v[2],
        2.0 * v[1] - v[2] - v[0],
        2.0 * v[2] - v[0] - v[1],
        6.0 * v[3],
        6.0 * v[4],
        6.0 * v[5],
    ]


def in_groups(lo, hi, size, body):
    full = (hi - lo) // size

    def step(i, carry):
        body(lo + size * i, size)
        return carry

    if full:
        lax.fori_loop(0, full, step, 0)
    if lo + size * full < hi:
        body(lo + size * full, hi - lo - size * full)


def own_kernel(mid, high, above, below, stats):
    lane = lanes()
    row = rows()

    def node(c, x):
        src, i, k = (mid, 8 * c + x, x % 4) if x < 8 else (high, 8 * c, 0)
        s = 1 if x < 8 else 2
        x = x % 8
        strip = src[64 + 4 * c + k]
        base = 64 if x >= 4 else 0
        far_strip = above[99 + 8 * s + 2 * c + x % 2]
        at = 64 * (x // 4) + (32 if k >= 2 else 0)
        real = None if s == 1 else within("gx", 1)
        upper = within("gy", 1)
        main = [masked(src[2 * i], real), masked(src[2 * i + 1], real), above[32 * s + i] * upper]
        strip, far_strip = masked(strip, real), far_strip * upper
        edge = [rolled(strip, 120 - base, 1), rolled(strip, 88 - base, 1), rolled(far_strip, 120 - at, 1)]
        after = [jnp.where(lane == 127, edge[t], rolled(main[t], -1, 1)) for t in range(3)]
        both = [after[t] + main[t] for t in range(3)]
        change = [after[t] - main[t] for t in range(3)]

        def follow(v):
            turned = [rolled(t, -1, 0) for t in v]
            return [jnp.where(row == 7, turned[t + 1], turned[t]) for t in range(2)]

        both_next, change_next = follow(both), follow(change)
        join2 = lambda v: jnp.concatenate(v[:2], axis=0)
        both, change, both_next, change_next = join2(both), join2(change), join2(both_next), join2(change_next)
        return both_next + both, both_next - both, change_next + change

    scores = []
    old = [node(c, 0) for c in range(3)]
    for x in range(8):
        new = [node(c, x + 1) for c in range(3)]
        values = scaled_stress(strain_of(new, old), 0.25 * shear_modulus)
        old = new
        dens = mid[48 + 2 * x : 50 + 2 * x].reshape(BY, 128)
        scores.append(power_scale * jnp.sqrt(dens * mises(values) + 1.0))
    most = functools.reduce(jnp.maximum, scores)
    top = jnp.max(most, axis=(0, 1), keepdims=True)
    total = sum(jnp.exp(score - top) for score in scores)
    total = jnp.sum(total, axis=(0, 1), keepdims=True)
    stats[0] = jnp.broadcast_to(top, (8, 128))
    stats[1] = jnp.broadcast_to(total, (8, 128))


def beside(body, ins, outs):
    def run(*refs):
        refs[ins + 1 + outs][...] = refs[ins][...]
        body(*refs[:ins], *refs[ins + 1 : ins + 1 + outs], *refs[ins + 2 + outs :])

    return run


def widen_kernel(mid, low, high, far, below, above, disp, line, edge, cells):
    sources = (low, mid, high)
    for p in range(NODES):
        for c in range(4 if p < CELLS else 3):
            value, beyond = unpacked(c, p, sources, far, below, above)
            if c == 3:
                cells[p] = value
            else:
                disp[c, p] = value
                line[c, p] = beyond[0]
                edge[c, p] = beyond[1]


def stress_kernel(disp, line, edge, cells, base, stress, highest, corners):
    def planes(p):
        return [corner_sums(disp[c, p], (line[c, p], edge[c, p])) for c in range(3)]

    put_corners(corners, planes(0))
    highest[...] = jnp.zeros((ROWS, 128), F32)

    def step(p, n):
        news = [get_corners(corners)] + [planes(p + 1 + j) for j in range(n)]
        most = highest[...]
        for j in range(n):
            values = scaled_stress(strain_of(news[j + 1], news[j]), 0.25 * shear_modulus)
            dens = cells[p + j]
            for i in range(6):
                base[i, p + j] = values[i]
            local = jnp.sqrt(dens * mises(values) + 1.0)
            stress[p + j] = local
            most = jnp.maximum(most, jnp.where(dens > 0.0, local, 0.0))
        highest[...] = most
        put_corners(corners, news[n])

    in_groups(0, CELLS, 2, step)


def load_kernel(base, cells, stress, highest, rhs, stiff, weight, explicit, field, reference, held, kept):
    top = power_scale * jnp.max(highest[...], axis=(0, 1), keepdims=True)
    reference[...] = jnp.broadcast_to(top, (8, 128))

    def element(p):
        dens = cells[p]
        values = [base[i, p] for i in range(6)]
        local = stress[p]
        factor = jnp.where(dens > 0.0, jnp.exp(power_scale * local - top), 0.0) / (2.0 * local)
        explicit[p] = factor * mises(values)
        part = scaled_stress(mises_slope(values), (0.25 * shear_modulus) * dens * factor)
        rigid = jnp.where(dens > 0.0, 0.01 + 0.99 * (dens * dens * dens), 0.0)
        stiff[p] = (shear_modulus / 16.0) * rigid
        return part, rigid

    part, rigid = element(0)
    for i in range(6):
        held[i] = part[i]
    kept[...] = rigid
    for c in range(3):
        field[c, 0] = jnp.zeros((ROWS, 128), F32)
        field[c, CELLS] = jnp.zeros((ROWS, 128), F32)

    def step(p, n):
        parts = [([held[i] for i in range(6)], kept[...])] + [element(p + j) for j in range(n)]
        for i in range(6):
            held[i] = parts[n][0][i]
        kept[...] = parts[n][1]
        for j in range(n):
            load = forces(parts[j][0], parts[j + 1][0])
            total = parts[j][1] + parts[j + 1][1]
            total = total + y_prev(total)
            total = total + z_prev(total)
            own = jnp.where(cells[p + j] > 0.0, damping / (diag_factor * total + shift_term), 0.0)
            weight[p + j] = own
            for c in range(3):
                value = own * load[c]
                rhs[c, p + j] = value
                field[c, p + j] = value

    in_groups(1, CELLS, GROUP, step)


def sweep_kernel(lo, hi, start, rhs, stiff, weight, field, held, corners):
    def planes(p):
        return [corner_sums(v) for v in get3(start, p)]

    def element(new, old, p):
        return scaled_stress(strain_of(new, old), stiff[p])

    first, second = planes(lo - 1), planes(lo)
    part = element(second, first, lo - 1)
    for i in range(6):
        held[i] = part[i]
    put_corners(corners, second)

    def step(p, n):
        news = [get_corners(corners)] + [planes(p + 1 + j) for j in range(n)]
        put_corners(corners, news[n])
        part = [held[i] for i in range(6)]
        for j in range(n):
            here = element(news[j + 1], news[j], p + j)
            force = forces(part, here)
            part = here
            own = weight[p + j]
            keep = 1.0 - shift_term * own
            for c in range(3):
                field[c, p + j] = keep * start[c, p + j] + rhs[c, p + j] - own * force[c]
        for i in range(6):
            held[i] = part[i]

    count = -(-(hi + 1 - lo) // GROUP) * GROUP
    in_groups(lo, lo + count, GROUP, step)


def positions(axis, length, cell):
    whole = lax.axis_size(axis) * length
    place = lax.axis_index(axis) * length + cell
    return lambda o: ((place + o >= 0) & (place + o < whole)).astype(F32)


def final_kernel(field, explicit, base, cells, reference, everyone, adjoint, sens, aggregate, corners, near, side, out):
    elements = BX * BY * BZ * lax.axis_size("gx") * lax.axis_size("gy") * lax.axis_size("gz")
    top, total = everyone[0], everyone[1]
    scale = jnp.exp(reference[...] - top) / total * float(elements)
    aggregate[...] = ((top + jnp.log(total)) / power_scale)[0:1, 0:1]
    scale = jnp.broadcast_to(scale[0:1, 0:1], (BY, 128))
    for c in range(3):
        for p in range(8):
            adjoint[c, p] = scale * field[c, 8 + p, 8:24, :]

    row = lax.broadcasted_iota(jnp.int32, (ROWS, 128), 0)
    lane = lax.broadcasted_iota(jnp.int32, (ROWS, 128), 1)
    group, place = lane // 32, lane % 32
    main = row < 32
    y_cell = jnp.where(main, row - 8, 8 * group + row - 40)
    z_cell = jnp.where(main, lane, jnp.where(place < 16, 121 + place, place - 24))
    in_y, in_z = positions("gy", BY, y_cell), positions("gz", BZ, z_cell)
    ys, zs = {o: in_y(o) for o in range(-2, 3)}, {o: in_z(o) for o in range(-2, 3)}
    beside = ys[-1] + ys[1]
    across = zs[-1] + zs[1]
    ones = beside * zs[0] + ys[0] * across
    diagonal = beside * across
    twos = (ys[-2] + ys[2]) * zs[0] + ys[0] * (zs[-2] + zs[2])
    centre = ys[0] * zs[0]
    near_0 = 2.5 * centre + W1 * ones + W2 * diagonal + W4 * twos
    near_1 = W1 * centre + W2 * ones + W3 * diagonal
    near_2 = W4 * centre

    def planes(p):
        return [corner_sums(v) for v in get3(field, p)]

    put_corners(corners, planes(6))

    def step(p, n):
        news = [get_corners(corners)] + [planes(p + 1 + j) for j in range(n)]
        put_corners(corners, news[n])
        for j in range(n):
            q = p + j
            strain = strain_of(news[j + 1], news[j])
            dens = cells[q]
            worked = base[0, q] * strain[0]
            for i in range(1, 6):
                worked = worked + base[i, q] * strain[i]
            raw = explicit[q] - (0.25 * 2.97) * dens * dens * worked
            in_x = positions("gx", BX, q - 8)
            hsum = near_0 + near_1 * (in_x(-1) + in_x(1)) + near_2 * (in_x(-2) + in_x(2))
            value = jnp.where(dens > 0.0, raw / jnp.where(dens > 0.0, hsum, 1.0), 0.0)
            above, under = z_next(value), z_prev(value)
            left, right = y_next(value), y_prev(value)
            row_pair = above + under
            unit = row_pair + (left + right)
            corner = y_next(row_pair) + y_prev(row_pair)
            two = z_next(above) + z_prev(under) + y_next(left) + y_prev(right)
            near[q - 6] = (2.5 * value + W1 * unit + W2 * corner + W4 * two)[8:24]
            side[q - 6] = (W1 * value + W2 * unit + W3 * corner)[8:24]
            out[q - 6] = (W4 * value)[8:24]

    in_groups(6, 18, GROUP, step)
    for p in range(8):
        q = p + 2
        sens[p] = scale * (near[q] + (side[q - 1] + side[q + 1]) + (out[q - 2] + out[q + 2]))


def passed(block, axis, distance):
    count = lax.axis_size(axis)
    return lax.ppermute(block, axis, [(i, (i + distance) % count) for i in range(count)])


def within(axis, distance):
    place = lax.axis_index(axis) + distance
    return ((place >= 0) & (place < lax.axis_size(axis))).astype(F32)


def merged(mine, other):
    larger = jnp.maximum(mine[0], other[0])
    gap = jnp.exp(jnp.minimum(mine[0], other[0]) - larger)
    first = mine[0] >= other[0]
    total = jnp.where(first, mine[1], other[1]) + jnp.where(first, other[1], mine[1]) * gap
    return jnp.stack([larger, total])


def on_device(displacement, density):
    plane = (ROWS, 128)
    main = jnp.concatenate([displacement.reshape(48, 8, 128), density.reshape(16, 8, 128)], axis=0)
    main = lax.optimization_barrier(main)
    up, down, inner, first = kernel_call(pack_z, [(16, 8, 128)] * 3 + [(6, 8, 128)], "pack_z")(main)
    below_z, above_z = passed(up, "gz", 1), passed(down, "gz", -1)
    strips = inner + below_z * within("gz", -1) + above_z * within("gz", 1)
    mid = jnp.concatenate([main, strips], axis=0)
    far = jnp.concatenate([first, strips[0:1], strips[4:5], strips[8:9]], axis=0)
    low, high, far = passed(mid, "gx", 1), passed(mid, "gx", -1), passed(far, "gx", -2)
    up, down = kernel_call(pack_y, [(126, 8, 128), (141, 8, 128)], "pack_y")(mid, low, high, far)
    below, above = passed(up, "gy", 1), passed(down, "gy", -1)
    (known,) = kernel_call(own_kernel, [(2, 8, 128)], "own")(mid, high, above, below)
    rounds = iter([("gy", 1), ("gx", 4), ("gx", 2), ("gx", 1), ("gy", 4), ("gy", 2), ("gz", 2), ("gz", 1)])

    def under(body, outs, name, scratch, aliases=None):
        def run(*args):
            nonlocal known
            axis, hop = next(rounds)
            other = lax.ppermute(known, axis, [(i, i ^ hop) for i in range(lax.axis_size(axis))])
            shapes = [*outs, (2, 8, 128)]
            call = kernel_call(beside(body, len(args), len(outs)), shapes, name, scratch, BUSY, aliases)
            *result, mine = call(*args, known)
            known = merged(mine, other)
            return result

        return run

    disp, line, edge, cells = under(
        widen_kernel,
        [(3, NODES, *plane), (3, NODES, 8, 128), (3, NODES, 8, 128), (CELLS, *plane)],
        "widen",
        [],
    )(mid, low, high, far, below, above)
    base, stress, highest = under(
        stress_kernel,
        [(6, CELLS, *plane), (CELLS, *plane), plane],
        "stress",
        [pltpu.VMEM((9, *plane), F32)],
    )(disp, line, edge, cells)
    rhs, stiff, weight, explicit, field, reference = under(
        load_kernel,
        [(3, CELLS, *plane), (CELLS, *plane), (CELLS, *plane), (CELLS, *plane), (3, NODES, *plane), (8, 128)],
        "load",
        [pltpu.VMEM((6, *plane), F32), pltpu.VMEM(plane, F32)],
    )(base, cells, stress, highest)
    for k in range(1, ITERS):
        (field,) = under(
            functools.partial(sweep_kernel, 1 + k, 23 - k),
            [(3, NODES, *plane)],
            f"sweep{k}",
            [pltpu.VMEM((6, *plane), F32), pltpu.VMEM((9, *plane), F32)],
            {0: 0},
        )(field, rhs, stiff, weight)
    everyone = known
    adjoint, sens, aggregate = kernel_call(
        final_kernel,
        [(3, BX, BY, BZ), (BX, BY, BZ), (1, 1)],
        "final",
        [
            pltpu.VMEM((9, *plane), F32),
            pltpu.VMEM((12, BY, 128), F32),
            pltpu.VMEM((12, BY, 128), F32),
            pltpu.VMEM((12, BY, 128), F32),
        ],
    )(field, explicit, base, cells, reference, everyone)
    return aggregate.reshape(()), adjoint, sens


def solution(mesh):
    placed = (P(None, "gx", "gy", "gz"), P("gx", "gy", "gz"))
    return jax.shard_map(
        on_device,
        mesh=mesh,
        in_specs=placed,
        out_specs=(P(), P(None, "gx", "gy", "gz"), P("gx", "gy", "gz")),
        check_vma=False,
    )
```
